128 devices in a mesh: time: 16 (over z, y_lo, core), chan: 8 (over y_hi, x).
Axes of the slice: x: 4, y: 4 (y_hi: 2, y_lo: 2; y = y_hi * 2 + y_lo), z: 4, core: 2. Of those that a mesh axis runs over, the one named last changes fastest.
Arguments:
- fade_rate: float32 [1, 8192, 4096], P(None, 'time', 'chan'), may hold values from 0.2 to 2
- update_in: bfloat16 [1, 8192, 4096], P(None, 'time', 'chan'), may hold values from -6 to 6
- norm_gain: float32 [4096], P('chan'), may hold values from 0.25 to 1.75
Outputs:
- mixed_out: bfloat16 [1, 8192, 4096], P(None, 'time', 'chan')
The draws below stay inside these ranges and needn't reach their ends.
All inputs are finite; a program needn't handle non-finite values.
Results may differ from the reference program's by a relative error of at most 0.001.
Values sent between devices are 32-bit elements; how exact they have to be, the bound alone decides.
No kernel may reach another device: no remote copies, remote signals or barrier semaphores. Data moves between devices by JAX's collectives and lax.ppermute only.
A program may use at most 64 MiB of HBM per device.

```python
import jax
import jax.numpy as jnp
from jax import lax

BATCH = 1
CHANNELS = 4096
LENGTH = 8192


def block_levels(rng, shape, cuts, low, largest):
    level = 1.0
    for dim, shards_of in cuts:
        draws = jax.random.uniform(jax.random.fold_in(jax.random.fold_in(rng, 6), dim), (shards_of,), jnp.float32, low / len(cuts), largest / len(cuts))
        level = level * jnp.repeat(jnp.exp(draws), shape[dim] // shards_of).reshape((-1,) + (1,) * (len(shape) - 1 - dim))
    return level


def normal_values(own_key, shape, spread, most, split=(), held_as=jnp.bfloat16):
    gain = block_levels(own_key, shape, split, -0.22, 0.18) if split else 1.0
    result = jax.random.normal(own_key, shape, jnp.float32) * spread * gain
    return jnp.minimum(jnp.maximum(result, -most), most).astype(held_as)


def setup_inputs(seed: int = 0) -> dict:
    streams_of = jax.random.split(jax.random.key(seed), 4)
    fade_rate = jnp.clip(0.2 + 1.8 * jax.random.uniform(streams_of[0], (BATCH, LENGTH, CHANNELS), jnp.float32) ** block_levels(streams_of[0], (BATCH, LENGTH, CHANNELS), ((1, 16), (2, 8)), -0.2, 0.2), 0.2, 2.0)
    update_in = normal_values(streams_of[1], (BATCH, LENGTH, CHANNELS), 1.0, 6.0, ((1, 16), (2, 8)))
    norm_gain = jnp.clip(1.0 + 0.15 * jax.random.normal(streams_of[2], (CHANNELS,), jnp.float32), 0.25, 1.75)
    return dict(fade_rate=fade_rate, update_in=update_in, norm_gain=norm_gain)


def join_pair(earlier, later):
    return (earlier[0] * later[0], later[0] * earlier[1] + later[1])

def reference(fade_rate, update_in, norm_gain):
    keep = jnp.exp(-fade_rate / LENGTH)
    push = update_in.astype(jnp.float32) * LENGTH ** (-0.5)
    forward = lax.associative_scan(join_pair, (keep, push), axis=1)[1]
    backward = lax.associative_scan(join_pair, (keep, push), axis=1, reverse=True)[1]
    states = forward + backward
    power = lax.optimization_barrier(jnp.mean(states * states, axis=-1, keepdims=True))
    mixed_out = (states * lax.rsqrt(power + 1e-06) * norm_gain).astype(jnp.bfloat16)
    return mixed_out
```

```python
import functools

import jax
import jax.numpy as jnp
from jax import lax
from jax.experimental import pallas as pl
from jax.experimental.pallas import tpu as pltpu
from jax.sharding import PartitionSpec as P

LANES = 128
SUBLANES = 8
BLOCK = 256


def dot(a, b):
    return jnp.dot(a, b, preferred_element_type=jnp.float32)


def rows_of(row):
    return [row[:, k : k + LANES] for k in range(0, row.shape[1], LANES)]


def local_kernel(total_length, rate_hbm, update_hbm, gain_hbm, local, fall, rise, stats, send, rate, update, gain, arrived):
    blocks = rate.shape[0] // BLOCK
    count = send.shape[0]
    me = lax.axis_index("time")
    copies = []
    for k in range(blocks):
        span = pl.ds(k * BLOCK, BLOCK)
        copies.append(pltpu.make_async_copy(rate_hbm.at[span], rate.at[span], arrived.at[0, k]))
        copies.append(pltpu.make_async_copy(update_hbm.at[span], update.at[span], arrived.at[1, k]))
    copies.append(pltpu.make_async_copy(gain_hbm, gain, arrived.at[0, blocks]))
    for copy in copies:
        copy.start()
    line = lax.broadcasted_iota(jnp.int32, (BLOCK, BLOCK), 0)
    column = lax.broadcasted_iota(jnp.int32, (BLOCK, BLOCK), 1)
    lower = jnp.where(line >= column, 1.0, 0.0).astype(jnp.bfloat16)
    upper = jnp.where(line <= column, 1.0, 0.0).astype(jnp.bfloat16)
    ends = []
    for k in range(blocks):
        span = pl.ds(k * BLOCK, BLOCK)
        copies[2 * k].wait()
        step = rate[span, :] * (1.0 / total_length)
        high = step.astype(jnp.bfloat16)
        low = (step - high.astype(jnp.float32)).astype(jnp.bfloat16)
        spent = dot(lower, high) + dot(lower, low)
        down = jnp.exp(-spent)
        up = jnp.exp(spent)
        half = 0.5 * step * step
        rising = up * (1.0 - step + half)
        falling = down * (1.0 + step + half)
        copies[2 * k + 1].wait()
        push_half = update[span, :]
        push = push_half.astype(jnp.float32)
        ahead = (up - 1.0) * push
        behind = (falling - 1.0) * push
        ends.append(
            (
                down[BLOCK - 1 :, :],
                down[BLOCK - 1 :, :] * jnp.sum(push + ahead, axis=0, keepdims=True),
                jnp.sum(push + behind, axis=0, keepdims=True),
            )
        )
        earlier = dot(lower, push_half) + dot(lower, ahead.astype(jnp.bfloat16))
        later = dot(upper, push_half) + dot(upper, behind.astype(jnp.bfloat16))
        local[span, :] = down * earlier + rising * later
        fall[span, :] = down
        rise[span, :] = rising
    (keep_0, forward_0, backward_0), (keep_1, forward_1, backward_1) = ends
    keep = keep_0 * keep_1
    forward = keep_1 * forward_0 + forward_1
    backward = backward_0 + keep_0 * backward_1
    copies[-1].wait()
    row = gain[...]
    stats[...] = jnp.concatenate([keep_0, forward_0, keep_1, backward_1, row, row, row, row], axis=0)
    to_later = jnp.concatenate(rows_of(keep) + rows_of(forward), axis=0)
    to_earlier = jnp.concatenate(rows_of(keep) + rows_of(backward), axis=0)
    for peer in range(count):
        send[peer] = jnp.where(peer > me, to_later, to_earlier)


def states_kernel(came, local, fall, rise, stats, states, send):
    count = came.shape[0]
    me = lax.axis_index("time")
    parts = [came[peer] for peer in range(count)]
    ends = [pltpu.roll(part, 4, axis=0) for part in parts]
    before = jnp.zeros((SUBLANES, LANES), jnp.float32)
    after = before
    for k in range(count):
        peer = count - 1 - k
        before = jnp.where(k < me, parts[k] * before + ends[k], before)
        after = jnp.where(peer > me, parts[peer] * after + ends[peer], after)
    before = jnp.concatenate([before[k : k + 1] for k in range(4)], axis=1)
    after = jnp.concatenate([after[k : k + 1] for k in range(4)], axis=1)
    keep_0, forward_0, keep_1, backward_1 = (stats[k : k + 1, :] for k in range(4))
    gain = stats[4:5, :]
    entering = [
        (before, keep_0 * (keep_1 * after + backward_1)),
        (keep_0 * before + forward_0, keep_1 * after),
    ]
    lane = lax.broadcasted_iota(jnp.int32, (SUBLANES, LANES), 1)
    power = jnp.zeros((SUBLANES, LANES), jnp.float32)
    for k in range(local.shape[0] // SUBLANES):
        span = pl.ds(k * SUBLANES, SUBLANES)
        first, second = entering[k * SUBLANES // BLOCK]
        state = local[span, :] + fall[span, :] * first + rise[span, :] * second
        states[span, :] = state * gain
        square = state * state
        square = functools.reduce(jnp.add, rows_of(square))
        power = jnp.where(lane == k, jnp.sum(square, axis=1, keepdims=True), power)
    for peer in range(send.shape[0]):
        send[peer] = power


def norm_kernel(scale, channels, came, states, mixed_hbm, mixed, left):
    power = functools.reduce(jnp.add, [came[peer] for peer in range(came.shape[0])])
    factor = lax.rsqrt(power * (scale * scale / channels) + 1e-6) * scale
    pieces = left.shape[0]
    height = states.shape[0] // pieces
    copies = []
    for piece in range(pieces):
        for k in range(piece * height // 16, (piece + 1) * height // 16):
            halves = []
            for j in (2 * k, 2 * k + 1):
                state = states[pl.ds(j * SUBLANES, SUBLANES), :]
                halves.append(state * factor[:, j : j + 1])
            mixed[pl.ds(16 * k, 16), :] = jnp.concatenate(halves, axis=0).astype(jnp.bfloat16)
        span = pl.ds(piece * height, height)
        copy = pltpu.make_async_copy(mixed.at[span], mixed_hbm.at[span], left.at[piece])
        copy.start()
        copies.append(copy)
    for copy in copies:
        copy.wait()


VMEM = pl.BlockSpec(memory_space=pltpu.VMEM)
HBM = pl.BlockSpec(memory_space=pltpu.HBM)
PARAMS = pltpu.CompilerParams(vmem_limit_bytes=16 << 20)


def placed(space, *arrays):
    return [pltpu.with_memory_space_constraint(array, space) for array in arrays]


def per_device(fade_rate, update_in, norm_gain):
    time, chan = lax.axis_size("time"), lax.axis_size("chan")
    length, width = fade_rate.shape[1:]
    total_length = length * time
    full = pltpu.VMEM((length, width), jnp.float32)
    local, fall, rise, stats, send = pl.pallas_call(
        functools.partial(local_kernel, total_length),
        out_shape=(full, full, full, pltpu.VMEM((SUBLANES, width), jnp.float32), pltpu.VMEM((time, SUBLANES, LANES), jnp.float32)),
        in_specs=[HBM] * 3,
        out_specs=(VMEM,) * 5,
        scratch_shapes=[
            pltpu.VMEM((length, width), jnp.float32),
            pltpu.VMEM((length, width), jnp.bfloat16),
            pltpu.VMEM((1, width), jnp.float32),
            pltpu.SemaphoreType.DMA((2, length // BLOCK + 1)),
        ],
        compiler_params=PARAMS,
        name="local",
    )(*placed(pltpu.HBM, fade_rate[0], update_in[0], norm_gain[None]))
    came = lax.all_to_all(send, "time", 0, 0, tiled=True)
    states, send = pl.pallas_call(
        states_kernel,
        out_shape=(full, pltpu.VMEM((chan, SUBLANES, LANES), jnp.float32)),
        in_specs=[VMEM] * 5,
        out_specs=(VMEM,) * 2,
        compiler_params=PARAMS,
        name="states",
    )(*placed(pltpu.VMEM, came, local, fall, rise, stats))
    came = lax.all_to_all(send, "chan", 0, 0, tiled=True)
    mixed = pl.pallas_call(
        functools.partial(norm_kernel, float(total_length) ** -0.5, width * chan),
        out_shape=jax.ShapeDtypeStruct((length, width), jnp.bfloat16),
        in_specs=[VMEM] * 2,
        out_specs=HBM,
        scratch_shapes=[pltpu.VMEM((length, width), jnp.bfloat16), pltpu.SemaphoreType.DMA((4,))],
        compiler_params=PARAMS,
        name="norm",
    )(*placed(pltpu.VMEM, came, states))
    return mixed[None]


def solution(mesh):
    shard = P(None, "time", "chan")
    return jax.shard_map(
        per_device, mesh=mesh, in_specs=(shard, shard, P("chan")), out_specs=shard, check_vma=False
    )
```

```python
import functools

import jax
import jax.numpy as jnp
from jax import lax
from jax.experimental import pallas as pl
from jax.experimental.pallas import tpu as pltpu
from jax.sharding import PartitionSpec as P


LANES = 128
BLOCK = 256
Z_ROUND = ((2, 0, 3, 1), (3, 2, 1, 0), (1, 3, 0, 2))
X_ROUND = ((3, 0, 1, 2), (2, 3, 0, 1), (1, 2, 3, 0))


def dot(a, b):
    return jnp.dot(a, b, preferred_element_type=jnp.float32)


def rows_of(row):
    return [row[:, k : k + LANES] for k in range(0, row.shape[1], LANES)]


def wide(tile):
    return jnp.concatenate([tile[k : k + 1] for k in range(4)], axis=1)


def my_place():
    me = lax.axis_index("time")
    return me // 4, (me // 2) % 2, me % 2


def unpacked(packet):
    first, second = packet[:8], packet[8:]
    return first, pltpu.roll(first, 4, axis=0), second


def packed(keep, forward, backward):
    return jnp.concatenate([keep[:4], forward[:4], backward[:4], keep[:4]], axis=0)


def joined(earlier, later):
    keep_0, forward_0, backward_0 = earlier
    keep_1, forward_1, backward_1 = later
    return keep_0 * keep_1, keep_1 * forward_0 + forward_1, backward_0 + keep_0 * backward_1


def chosen(take, yes, no):
    return tuple(jnp.where(take, a, b) for a, b in zip(yes, no))


def ends_kernel(total_length, rate_hbm, update_hbm, gain_hbm, fall, rise, ahead, behind, push, stats, packet, rate, gain, arrived):
    blocks = rate.shape[0] // BLOCK
    copies = []
    for k in range(blocks):
        span = pl.ds(k * BLOCK, BLOCK)
        copies.append(pltpu.make_async_copy(rate_hbm.at[span], rate.at[span], arrived.at[0, k]))
        copies.append(pltpu.make_async_copy(update_hbm.at[span], push.at[span], arrived.at[1, k]))
    copies.append(pltpu.make_async_copy(gain_hbm, gain, arrived.at[0, blocks]))
    for copy in copies:
        copy.start()
    line = lax.broadcasted_iota(jnp.int32, (BLOCK, BLOCK), 0)
    column = lax.broadcasted_iota(jnp.int32, (BLOCK, BLOCK), 1)
    lower = jnp.where(line >= column, 1.0, 0.0).astype(jnp.bfloat16)
    ends = []
    for k in range(blocks):
        span = pl.ds(k * BLOCK, BLOCK)
        copies[2 * k].wait()
        step = rate[span, :] * (1.0 / total_length)
        high = step.astype(jnp.bfloat16)
        low = (step - high.astype(jnp.float32)).astype(jnp.bfloat16)
        spent = dot(lower, high) + dot(lower, low)
        down = jnp.exp(-spent)
        up = jnp.exp(spent)
        half = 0.5 * step * step
        copies[2 * k + 1].wait()
        update = push[span, :].astype(jnp.float32)
        more = (up - 1.0) * update
        less = (down * (1.0 + step + half) - 1.0) * update
        last = down[BLOCK - 1 :, :]
        ends.append(
            (
                last,
                last * jnp.sum(update + more, axis=0, keepdims=True),
                jnp.sum(update + less, axis=0, keepdims=True),
            )
        )
        ahead[span, :] = more.astype(jnp.bfloat16)
        behind[span, :] = less.astype(jnp.bfloat16)
        fall[span, :] = down
        rise[span, :] = up * (1.0 - step + half)
    keep, forward, backward = joined(*ends)
    copies[-1].wait()
    row = gain[...]
    stats[...] = jnp.concatenate([ends[0][0], ends[0][1], ends[1][0], ends[1][2], row, row, row, row], axis=0)
    packet[...] = jnp.concatenate(rows_of(keep) + rows_of(forward) + rows_of(backward) + rows_of(keep), axis=0)


def local_kernel(fall, rise, ahead, behind, push, local):
    line = lax.broadcasted_iota(jnp.int32, (BLOCK, BLOCK), 0)
    column = lax.broadcasted_iota(jnp.int32, (BLOCK, BLOCK), 1)
    lower = jnp.where(line >= column, 1.0, 0.0).astype(jnp.bfloat16)
    upper = jnp.where(line <= column, 1.0, 0.0).astype(jnp.bfloat16)
    for k in range(push.shape[0] // BLOCK):
        span = pl.ds(k * BLOCK, BLOCK)
        update = push[span, :]
        earlier = dot(lower, update) + dot(lower, ahead[span, :])
        later = dot(upper, update) + dot(upper, behind[span, :])
        local[span, :] = fall[span, :] * earlier + rise[span, :] * later


def join_kernel(digit, own, came, packet):
    own, came = unpacked(own[...]), unpacked(came[...])
    second = my_place()[digit] == 1
    packet[...] = packed(*joined(chosen(second, came, own), chosen(second, own, came)))


def entering_kernel(pair, came_0, came_1, came_2, neighbour, entering):
    z, y_lo, _ = my_place()
    packets = [pair[...]] + [ref[...] for ref in (came_0, came_1, came_2)]
    sources = [z]
    for sends in Z_ROUND:
        source = sends.index(3)
        for k in range(3):
            source = jnp.where(z == k, sends.index(k), source)
        sources.append(source)
    before = jnp.zeros((8, LANES), jnp.float32)
    after = before
    ordered = []
    for k in range(4):
        packet = packets[0]
        for source, other in zip(sources[1:], packets[1:]):
            packet = jnp.where(source == k, other, packet)
        ordered.append(unpacked(packet))
    for k in range(4):
        keep, forward, _ = ordered[k]
        before = jnp.where(k < z, keep * before + forward, before)
        keep, _, backward = ordered[3 - k]
        after = jnp.where(3 - k > z, keep * after + backward, after)
    keep, forward, backward = unpacked(neighbour[...])
    before = jnp.where(y_lo == 1, keep * before + forward, before)
    after = jnp.where(y_lo == 0, keep * after + backward, after)
    entering[...] = jnp.concatenate([before, after], axis=0)


def states_kernel(own, came, partner, local, fall, rise, stats, states, power_out):
    core = my_place()[2]
    entering = jnp.where(core == 1, own[...], came[...])
    before, after = entering[:8], entering[8:]
    keep, forward, backward = unpacked(partner[...])
    before = wide(jnp.where(core == 1, keep * before + forward, before))
    after = wide(jnp.where(core == 0, keep * after + backward, after))
    keep_0, forward_0, keep_1, backward_1 = (stats[k : k + 1, :] for k in range(4))
    gain = stats[4:5, :]
    at_blocks = [
        (before, keep_0 * (keep_1 * after + backward_1)),
        (keep_0 * before + forward_0, keep_1 * after),
    ]
    lane = lax.broadcasted_iota(jnp.int32, (8, LANES), 1)
    power = jnp.zeros((8, LANES), jnp.float32)
    for k in range(local.shape[0] // 8):
        span = pl.ds(8 * k, 8)
        first, second = at_blocks[8 * k // BLOCK]
        state = local[span, :] + fall[span, :] * first + rise[span, :] * second
        states[span, :] = state * gain
        square = functools.reduce(jnp.add, rows_of(state * state))
        power = jnp.where(lane == k, jnp.sum(square, axis=1, keepdims=True), power)
    power_out[...] = jnp.where(core == 1, pltpu.roll(power, LANES // 2, axis=1), power)


def norm_kernel(mine, scale, channels, power, states, *refs):
    mixed_hbm, mixed, left = refs[-3:]

    @pl.when(my_place()[2] == mine)
    def _():
        factor = lax.rsqrt(power[...] * (scale * scale / channels) + 1e-6) * scale
        pieces = left.shape[0]
        height = states.shape[0] // pieces
        copies = []
        for piece in range(pieces):
            for k in range(piece * height // 16, (piece + 1) * height // 16):
                halves = []
                for j in (2 * k, 2 * k + 1):
                    place = j + mine * (LANES // 2)
                    halves.append(states[pl.ds(8 * j, 8), :] * factor[:, place : place + 1])
                mixed[pl.ds(16 * k, 16), :] = jnp.concatenate(halves, axis=0).astype(jnp.bfloat16)
            span = pl.ds(piece * height, height)
            copy = pltpu.make_async_copy(mixed.at[span], mixed_hbm.at[span], left.at[piece])
            copy.start()
            copies.append(copy)
        for copy in copies:
            copy.wait()


VMEM = pl.BlockSpec(memory_space=pltpu.VMEM)
HBM = pl.BlockSpec(memory_space=pltpu.HBM)
PARAMS = pltpu.CompilerParams(vmem_limit_bytes=16 << 20)
SPACES = ("time", "chan")


def placed(space, *arrays):
    return [pltpu.with_memory_space_constraint(array, space) for array in arrays]


def call(kernel, outs, name, *arrays):
    return pl.pallas_call(
        kernel,
        out_shape=tuple(outs),
        in_specs=[VMEM] * len(arrays),
        out_specs=(VMEM,) * len(outs),
        compiler_params=PARAMS,
        name=name,
    )(*placed(pltpu.VMEM, *arrays))


def moved(value, target):
    pairs = []
    for place in range(128):
        t, c = place // 8, place % 8
        z, y_lo, core, y_hi, x = target(t // 4, (t // 2) % 2, t % 2, c // 4, c % 4)
        pairs.append((place, (z * 4 + y_lo * 2 + core) * 8 + y_hi * 4 + x))
    return lax.ppermute(value, SPACES, pairs)


def between_cores(value):
    return moved(value, lambda z, y_lo, core, y_hi, x: (z, y_lo, 1 - core, y_hi, x))


def relayed(value, target):
    return moved(
        value,
        lambda z, y_lo, core, y_hi, x: (
            (*target(z, y_lo, y_hi, x)[:2], 1, *target(z, y_lo, y_hi, x)[2:]) if core else (z, 1 - y_lo, 0, y_hi, x)
        ),
    )


def per_device(fade_rate, update_in, norm_gain):
    time, chan = lax.axis_size("time"), lax.axis_size("chan")
    length, width = fade_rate.shape[1:]
    total_length = length * time
    full = pltpu.VMEM((length, width), jnp.float32)
    half = pltpu.VMEM((length, width), jnp.bfloat16)
    packet = pltpu.VMEM((16, LANES), jnp.float32)
    tile = pltpu.VMEM((8, LANES), jnp.float32)
    fall, rise, ahead, behind, push, stats, own = pl.pallas_call(
        functools.partial(ends_kernel, total_length),
        out_shape=(full, full, half, half, half, pltpu.VMEM((8, width), jnp.float32), packet),
        in_specs=[HBM] * 3,
        out_specs=(VMEM,) * 7,
        scratch_shapes=[
            pltpu.VMEM((length, width), jnp.float32),
            pltpu.VMEM((1, width), jnp.float32),
            pltpu.SemaphoreType.DMA((2, length // BLOCK + 1)),
        ],
        compiler_params=PARAMS,
        name="ends",
    )(*placed(pltpu.HBM, fade_rate[0], update_in[0], norm_gain[None]))

    partner = between_cores(own)
    (chip,) = call(functools.partial(join_kernel, 2), [packet], "chip", own, partner)
    neighbour = relayed(chip, lambda z, y_lo, y_hi, x: (z, 1 - y_lo, y_hi, x))
    (pair,) = call(functools.partial(join_kernel, 1), [packet], "pair", chip, neighbour)
    around = [relayed(pair, lambda z, y_lo, y_hi, x, to=to: (to[z], y_lo, y_hi, x)) for to in Z_ROUND]
    (local,) = call(local_kernel, [full], "local", fall, rise, ahead, behind, push)
    (entering,) = call(entering_kernel, [packet], "entering", pair, *around, neighbour)
    came = between_cores(entering)
    states, power = call(states_kernel, [full, tile], "states", entering, came, partner, local, fall, rise, stats)

    power = power + between_cores(power)
    power = power + relayed(power, lambda z, y_lo, y_hi, x: (z, y_lo, 1 - y_hi, x))
    for part in [relayed(power, lambda z, y_lo, y_hi, x, to=to: (z, y_lo, y_hi, to[x])) for to in X_ROUND]:
        power = power + part
    came = between_cores(power)

    def norm(mine, power, *before):
        return pl.pallas_call(
            functools.partial(norm_kernel, mine, float(total_length) ** -0.5, width * chan),
            out_shape=jax.ShapeDtypeStruct((length, width), jnp.bfloat16),
            in_specs=[VMEM] * 2 + [HBM] * len(before),
            out_specs=HBM,
            input_output_aliases={2: 0} if before else {},
            scratch_shapes=[pltpu.VMEM((length, width), jnp.bfloat16), pltpu.SemaphoreType.DMA((4,))],
            compiler_params=PARAMS,
            name=f"norm_{mine}",
        )(*placed(pltpu.VMEM, power, states), *placed(pltpu.HBM, *before))

    return norm(0, came, norm(1, power))[None]


def solution(mesh):
    shard = P(None, "time", "chan")
    return jax.shard_map(
        per_device, mesh=mesh, in_specs=(shard, shard, P("chan")), out_specs=shard, check_vma=False
    )
```

```python
import functools
import math

import jax
import jax.numpy as jnp
from jax import lax
from jax.experimental import pallas as pl
from jax.experimental.pallas import tpu as pltpu
from jax.sharding import PartitionSpec as P


LANES = 128
BLOCK = 256
Z_ROUND = ((1, 3, 0, 2), (3, 2, 1, 0), (2, 0, 3, 1))
X_ROUND = ((1, 2, 3, 0), (2, 3, 0, 1), (3, 0, 1, 2))


def dot(a, b):
    return jnp.dot(a, b, preferred_element_type=jnp.float32)


def rows_of(row):
    return [row[:, k : k + LANES] for k in range(0, row.shape[1], LANES)]


def triangle(keeps):
    shape = (BLOCK, BLOCK)
    kept = keeps(lax.broadcasted_iota(jnp.int32, shape, 0), lax.broadcasted_iota(jnp.int32, shape, 1))
    return jnp.where(kept, 1.0, 0.0).astype(jnp.bfloat16)


def wide(tile):
    return jnp.concatenate([tile[k : k + 1] for k in range(4)], axis=1)


def my_place():
    me = lax.axis_index("time")
    return me // 4, (me // 2) % 2, me % 2


def unpacked(packet):
    first, second = packet[:8], packet[8:]
    return first, pltpu.roll(first, 4, axis=0), second


def packed(keep, forward, backward):
    return jnp.concatenate([keep[:4], forward[:4], backward[:4], keep[:4]], axis=0)


def joined(earlier, later):
    keep_0, forward_0, backward_0 = earlier
    keep_1, forward_1, backward_1 = later
    return keep_0 * keep_1, keep_1 * forward_0 + forward_1, backward_0 + keep_0 * backward_1


def chosen(take, yes, no):
    return tuple(jnp.where(take, a, b) for a, b in zip(yes, no))


def ends_kernel(per_rate, rate_hbm, update_hbm, gain_hbm, rate, spent, push, stats, packet, gain, arrived):
    blocks = rate.shape[0] // BLOCK
    copies = []
    for k in range(blocks):
        span = pl.ds(k * BLOCK, BLOCK)
        copies.append(pltpu.make_async_copy(rate_hbm.at[span], rate.at[span], arrived.at[0, k]))
        copies.append(pltpu.make_async_copy(update_hbm.at[span], push.at[span], arrived.at[1, k]))
    copies.append(pltpu.make_async_copy(gain_hbm, gain, arrived.at[0, blocks]))
    for copy in copies:
        copy.start()
    lower = triangle(jnp.greater_equal)
    ends = []
    for k in range(blocks):
        span = pl.ds(k * BLOCK, BLOCK)
        copies[2 * k].wait()
        step = rate[span, :] * per_rate
        high = step.astype(jnp.bfloat16)
        low = (step - high.astype(jnp.float32)).astype(jnp.bfloat16)
        spent[span, :] = dot(lower, high) + dot(lower, low)
        copies[2 * k + 1].wait()
        forward = jnp.zeros((8, rate.shape[1]), jnp.float32)
        backward = forward
        for row in range(k * BLOCK, (k + 1) * BLOCK, 16):
            rows = pl.ds(row, 16)
            total = spent[rows, :]
            update = push[rows, :].astype(jnp.float32)
            more = jnp.exp2(total) * update
            less = jnp.exp2(rate[rows, :] * per_rate - total) * update
            forward = forward + (more[:8] + more[8:])
            backward = backward + (less[:8] + less[8:])
        keep = jnp.exp2(-spent[pl.ds((k + 1) * BLOCK - 8, 8), :][7:])
        ends.append((keep, keep * jnp.sum(forward, axis=0, keepdims=True), jnp.sum(backward, axis=0, keepdims=True)))
    keep, forward, backward = joined(*ends)
    copies[-1].wait()
    row = ends[0][0]
    stats[...] = jnp.concatenate([ends[0][0], ends[0][1], ends[1][0], ends[1][2], row, row, row, row], axis=0)
    packet[...] = jnp.concatenate(rows_of(keep) + rows_of(forward) + rows_of(backward) + rows_of(keep), axis=0)


def local_kernel(block, per_rate, rate, spent, push, *refs):
    fields, ahead, behind = refs[-3:]
    local, fall, rise = (fields.at[3 * block + k] for k in range(3))
    for row in range(0, BLOCK, 16):
        rows, here = pl.ds(block * BLOCK + row, 16), pl.ds(row, 16)
        total = spent[rows, :]
        before = total - rate[rows, :] * per_rate
        update = push[rows, :].astype(jnp.float32)
        fall[here, :] = jnp.exp2(-total)
        rise[here, :] = jnp.exp2(before)
        ahead[here, :] = ((jnp.exp2(total) - 1.0) * update).astype(jnp.bfloat16)
        behind[here, :] = ((jnp.exp2(-before) - 1.0) * update).astype(jnp.bfloat16)
    lower, upper = triangle(jnp.greater_equal), triangle(jnp.less_equal)
    update = push[pl.ds(block * BLOCK, BLOCK), :]
    earlier = dot(lower, update) + dot(lower, ahead[...])
    later = dot(upper, update) + dot(upper, behind[...])
    local[...] = fall[...] * earlier + rise[...] * later


def join_kernel(digit, own, came, _, packet):
    own, came = unpacked(own[...]), unpacked(came[...])
    second = my_place()[digit] == 1
    packet[...] = packed(*joined(chosen(second, came, own), chosen(second, own, came)))


def entering_kernel(pair, came_0, came_1, came_2, neighbour, entering):
    z, y_lo, _ = my_place()
    packets = [pair[...]] + [ref[...] for ref in (came_0, came_1, came_2)]
    sources = [z]
    for sends in Z_ROUND:
        source = sends.index(3)
        for k in range(3):
            source = jnp.where(z == k, sends.index(k), source)
        sources.append(source)
    before = jnp.zeros((8, LANES), jnp.float32)
    after = before
    ordered = []
    for k in range(4):
        packet = packets[0]
        for source, other in zip(sources[1:], packets[1:]):
            packet = jnp.where(source == k, other, packet)
        ordered.append(unpacked(packet))
    for k in range(4):
        keep, forward, _ = ordered[k]
        before = jnp.where(k < z, keep * before + forward, before)
        keep, _, backward = ordered[3 - k]
        after = jnp.where(3 - k > z, keep * after + backward, after)
    keep, forward, backward = unpacked(neighbour[...])
    before = jnp.where(y_lo == 1, keep * before + forward, before)
    after = jnp.where(y_lo == 0, keep * after + backward, after)
    entering[...] = jnp.concatenate([before, after], axis=0)


def entering_blocks(before, after, stats):
    before, after = wide(before), wide(after)
    keep_0, forward_0, keep_1, backward_1 = (stats[k : k + 1, :] for k in range(4))
    return (before, keep_0 * (keep_1 * after + backward_1)), (keep_0 * before + forward_0, keep_1 * after)


def filtered(fields, entering, use):
    for k in range(2 * BLOCK // 8):
        block, row = divmod(8 * k, BLOCK)
        local, fall, rise = (fields[3 * block + j, pl.ds(row, 8), :] for j in range(3))
        first, second = entering[block]
        use(k, local + fall * first + rise * second)


def power_kernel(entering, own, partner, fields, stats, gain, fields_0, stats_0, states, power_out):
    core = my_place()[2]

    @pl.when(core == 0)
    def _():
        power_out[...] = jnp.zeros((8, LANES), jnp.float32)

    @pl.when(core == 1)
    def _():
        before, after = entering[:8], entering[8:]
        lane = lax.broadcasted_iota(jnp.int32, (8, LANES), 1)
        power = [jnp.zeros((8, LANES), jnp.float32)]
        scale = gain[...]

        def add(place, state):
            square = functools.reduce(jnp.add, rows_of(state * state))
            power[0] = jnp.where(lane == place, jnp.sum(square, axis=1, keepdims=True), power[0])

        def keep_it(k, state):
            states[pl.ds(8 * k, 8), :] = state * scale
            add(LANES // 2 + k, state)

        keep, forward, _ = unpacked(partner[...])
        filtered(fields, entering_blocks(keep * before + forward, after, stats), keep_it)
        keep, _, backward = unpacked(own[...])
        filtered(fields_0, entering_blocks(before, keep * after + backward, stats_0), add)
        power_out[...] = power[0]


def states_kernel(came, partner, fields, stats, gain, states_1, states):
    @pl.when(my_place()[2] == 0)
    def _():
        before, after = came[:8], came[8:]
        keep, _, backward = unpacked(partner[...])
        scale = gain[...]

        def keep_it(k, state):
            states[pl.ds(8 * k, 8), :] = state * scale

        filtered(fields, entering_blocks(before, keep * after + backward, stats), keep_it)


def add_kernel(a, b, _, total):
    total[...] = a[...] + b[...]


def norm_kernel(mine, scale, channels, power, states, *refs):
    mixed_hbm, mixed, left = refs[-3:]

    @pl.when(my_place()[2] == mine)
    def _():
        factor = lax.rsqrt(power[...] * (scale * scale / channels) + 1e-6) * scale
        pieces = left.shape[0]
        height = states.shape[0] // pieces
        copies = []
        for piece in range(pieces):
            for k in range(piece * height // 16, (piece + 1) * height // 16):
                halves = []
                for j in (2 * k, 2 * k + 1):
                    place = j + mine * (LANES // 2)
                    halves.append(states[pl.ds(8 * j, 8), :] * factor[:, place : place + 1])
                mixed[pl.ds(16 * k, 16), :] = jnp.concatenate(halves, axis=0).astype(jnp.bfloat16)
            span = pl.ds(piece * height, height)
            copy = pltpu.make_async_copy(mixed.at[span], mixed_hbm.at[span], left.at[piece])
            copy.start()
            copies.append(copy)
        for copy in copies:
            copy.wait()


VMEM = pl.BlockSpec(memory_space=pltpu.VMEM)
HBM = pl.BlockSpec(memory_space=pltpu.HBM)
PARAMS = pltpu.CompilerParams(vmem_limit_bytes=16 << 20)
SPACES = ("time", "chan")


def placed(space, *arrays):
    return [pltpu.with_memory_space_constraint(array, space) for array in arrays]


def call(kernel, outs, *arrays, scratch=(), aliases={}):
    return pl.pallas_call(
        kernel,
        out_shape=tuple(outs),
        in_specs=[VMEM] * len(arrays),
        out_specs=(VMEM,) * len(outs),
        scratch_shapes=scratch,
        input_output_aliases=aliases,
        compiler_params=PARAMS,
    )(*placed(pltpu.VMEM, *arrays))


def moved(value, target):
    pairs = []
    for place in range(128):
        t, c = place // 8, place % 8
        z, y_lo, core, y_hi, x = target(t // 4, (t // 2) % 2, t % 2, c // 4, c % 4)
        pairs.append((place, (z * 4 + y_lo * 2 + core) * 8 + y_hi * 4 + x))
    return lax.ppermute(value, SPACES, pairs)


def between_cores(value):
    return moved(
        value, lambda z, y_lo, core, y_hi, x: (z, y_lo, 1 - core, y_hi, x))


def relayed(value, target):
    return moved(
        value,
        lambda z, y_lo, core, y_hi, x: (
            (*target(z, y_lo, y_hi, x)[:2], 1, *target(z, y_lo, y_hi, x)[2:]) if core else (z, 1 - y_lo, 0, y_hi, x)
        ),
    )


def per_device(fade_rate, update_in, norm_gain):
    time, chan = lax.axis_size("time"), lax.axis_size("chan")
    length, width = fade_rate.shape[1:]
    total_length = length * time
    per_rate = math.log2(math.e) / total_length
    full = pltpu.VMEM((length, width), jnp.float32)
    packet = pltpu.VMEM((16, LANES), jnp.float32)
    tile = pltpu.VMEM((8, LANES), jnp.float32)
    rate, spent, push, stats, own, gain = pl.pallas_call(
        functools.partial(ends_kernel, per_rate),
        out_shape=(
            full,
            full,
            pltpu.VMEM((length, width), jnp.bfloat16),
            pltpu.VMEM((8, width), jnp.float32),
            packet,
            pltpu.VMEM((1, width), jnp.float32),
        ),
        in_specs=[HBM] * 3,
        out_specs=(VMEM,) * 6,
        scratch_shapes=[pltpu.SemaphoreType.DMA((2, length // BLOCK + 1))],
        compiler_params=PARAMS,
        name="ends",
    )(*placed(pltpu.HBM, fade_rate[0], update_in[0], norm_gain[None]))

    def local(block, *others):
        half = pltpu.VMEM((BLOCK, width), jnp.bfloat16)
        return call(
            functools.partial(local_kernel, block, per_rate),
            [pltpu.VMEM((3 * length // BLOCK, BLOCK, width), jnp.float32)],
            rate,
            spent,
            push,
            *others,
            scratch=[half, half],
            aliases={3: 0} if others else {},
        )[0]

    first = local(0)
    fields = local(1, first)
    partner = between_cores(own)
    (chip,) = call(functools.partial(join_kernel, 2), [packet], own, partner, first)
    neighbour = relayed(chip, lambda z, y_lo, y_hi, x: (z, 1 - y_lo, y_hi, x))
    (pair,) = call(functools.partial(join_kernel, 1), [packet], chip, neighbour, fields)
    around = [relayed(pair, lambda z, y_lo, y_hi, x, to=to: (to[z], y_lo, y_hi, x)) for to in Z_ROUND]
    (entering,) = call(entering_kernel, [packet], pair, *around, neighbour)
    fields_0, stats_0 = between_cores(fields), between_cores(stats)
    came = between_cores(entering)
    states, power = call(power_kernel, [full, tile], entering, own, partner, fields, stats, gain, fields_0, stats_0)
    (states,) = call(states_kernel, [full], came, partner, fields, stats, gain, states, aliases={5: 0})

    def add(a, b, other):
        return call(add_kernel, [tile], a, b, other)[0]

    power = add(power, relayed(power, lambda z, y_lo, y_hi, x: (z, y_lo, 1 - y_hi, x)), states)
    for part in [relayed(power, lambda z, y_lo, y_hi, x, to=to: (z, y_lo, y_hi, to[x])) for to in X_ROUND]:
        power = power + part
    came = between_cores(power)

    def norm(mine, power, *before):
        return pl.pallas_call(
            functools.partial(norm_kernel, mine, float(total_length) ** -0.5, width * chan),
            out_shape=jax.ShapeDtypeStruct((length, width), jnp.bfloat16),
            in_specs=[VMEM] * 2 + [HBM] * len(before),
            out_specs=HBM,
            input_output_aliases={2: 0} if before else {},
            scratch_shapes=[pltpu.VMEM((length, width), jnp.bfloat16), pltpu.SemaphoreType.DMA((4,))],
            compiler_params=PARAMS,
        )(*placed(pltpu.VMEM, power, states), *placed(pltpu.HBM, *before))

    return norm(0, came, norm(1, power))[None]


def solution(mesh):
    shard = P(None, "time", "chan")
    return jax.shard_map(per_device, mesh=mesh, in_specs=(shard, shard, P("chan")), out_specs=shard, check_vma=False)
```

```python
import functools
import math

import jax
import jax.numpy as jnp
from jax import lax
from jax.experimental import pallas as pl
from jax.experimental.pallas import tpu as pltpu
from jax.sharding import PartitionSpec as P


LANES = 128
BLOCK = 256
Z_ROUND = ((1, 3, 0, 2), (3, 2, 1, 0), (2, 0, 3, 1))
X_ROUND = ((1, 3, 0, 2), (3, 2, 1, 0), (2, 0, 3, 1))


def dot(a, b):
    return jnp.dot(a, b, preferred_element_type=jnp.float32)


def rows_of(row):
    return [row[:, k : k + LANES] for k in range(0, row.shape[1], LANES)]


def triangle(keeps):
    shape = (BLOCK, BLOCK)
    kept = keeps(lax.broadcasted_iota(jnp.int32, shape, 0), lax.broadcasted_iota(jnp.int32, shape, 1))
    return jnp.where(kept, 1.0, 0.0).astype(jnp.bfloat16)


def wide(tile):
    return jnp.concatenate([tile[k : k + 1] for k in range(4)], axis=1)


def my_place():
    me = lax.axis_index("time")
    return me // 4, (me // 2) % 2, me % 2


def unpacked(packet):
    first, second = packet[:8], packet[8:]
    return first, pltpu.roll(first, 4, axis=0), second


def packed(keep, forward, backward):
    return jnp.concatenate([keep[:4], forward[:4], backward[:4], keep[:4]], axis=0)


def joined(earlier, later):
    keep_0, forward_0, backward_0 = earlier
    keep_1, forward_1, backward_1 = later
    return keep_0 * keep_1, keep_1 * forward_0 + forward_1, backward_0 + keep_0 * backward_1


def chosen(take, yes, no):
    return tuple(jnp.where(take, a, b) for a, b in zip(yes, no))


def ends_kernel(per_rate, rate_hbm, update_hbm, gain_hbm, rate, spent, push, stats, packet, gain, arrived):
    blocks = rate.shape[0] // BLOCK
    copies = []
    for k in range(blocks):
        span = pl.ds(k * BLOCK, BLOCK)
        copies.append(pltpu.make_async_copy(rate_hbm.at[span], rate.at[span], arrived.at[0, k]))
        copies.append(pltpu.make_async_copy(update_hbm.at[span], push.at[span], arrived.at[1, k]))
    copies.append(pltpu.make_async_copy(gain_hbm, gain, arrived.at[0, blocks]))
    for copy in copies:
        copy.start()
    half = BLOCK // 2
    line = lax.broadcasted_iota(jnp.int32, (half, BLOCK), 0)
    column = lax.broadcasted_iota(jnp.int32, (half, BLOCK), 1) % half
    twice_lower = jnp.where(line >= column, 1.0, 0.0).astype(jnp.bfloat16)
    ends = []
    for k in range(blocks):
        copies[2 * k].wait()
        so_far = 0.0
        for row in range(k * BLOCK, (k + 1) * BLOCK, half):
            span = pl.ds(row, half)
            step = rate[span, :] * per_rate
            high = step.astype(jnp.bfloat16)
            low = (step - high.astype(jnp.float32)).astype(jnp.bfloat16)
            spent[span, :] = dot(twice_lower, jnp.concatenate([high, low], axis=0)) + so_far
            so_far = spent[pl.ds(row + half - 8, 8), :][7:]
        copies[2 * k + 1].wait()
        forward = jnp.zeros((8, rate.shape[1]), jnp.float32)
        backward = forward
        for row in range(k * BLOCK, (k + 1) * BLOCK, 16):
            rows = pl.ds(row, 16)
            total = spent[rows, :]
            update = push[rows, :].astype(jnp.float32)
            more = jnp.exp2(total) * update
            less = jnp.exp2(rate[rows, :] * per_rate - total) * update
            forward = forward + (more[:8] + more[8:])
            backward = backward + (less[:8] + less[8:])
        keep = jnp.exp2(-spent[pl.ds((k + 1) * BLOCK - 8, 8), :][7:])
        ends.append((keep, keep * jnp.sum(forward, axis=0, keepdims=True), jnp.sum(backward, axis=0, keepdims=True)))
    keep, forward, backward = joined(*ends)
    copies[-1].wait()
    row = ends[0][0]
    stats[...] = jnp.concatenate([ends[0][0], ends[0][1], ends[1][0], ends[1][2], row, row, row, row], axis=0)
    packet[...] = jnp.concatenate(rows_of(keep) + rows_of(forward) + rows_of(backward) + rows_of(keep), axis=0)


def field(fields, block, k):
    return fields.at[pl.ds((3 * block + k) * BLOCK, BLOCK)]


def local_kernel(mine, blocks, per_rate, rate, spent, push, stats, *refs):
    fields, ahead, behind = refs[-3:]

    @pl.when(my_place()[2] == mine)
    def _():
        lower, upper = triangle(jnp.greater_equal), triangle(jnp.less_equal)
        for block in blocks:
            local, fall, rise = (field(fields, block, k) for k in range(3))
            for row in range(0, BLOCK, 16):
                rows, here = pl.ds(block * BLOCK + row, 16), pl.ds(row, 16)
                total = spent[rows, :]
                before = total - rate[rows, :] * per_rate
                update = push[rows, :].astype(jnp.float32)
                fall[here, :] = jnp.exp2(-total)
                rise[here, :] = jnp.exp2(before)
                ahead[here, :] = ((jnp.exp2(total) - 1.0) * update).astype(jnp.bfloat16)
                behind[here, :] = ((jnp.exp2(-before) - 1.0) * update).astype(jnp.bfloat16)
            update = push[pl.ds(block * BLOCK, BLOCK), :]
            earlier = dot(lower, update) + dot(lower, ahead[...])
            later = dot(upper, update) + dot(upper, behind[...])
            local[...] = fall[...] * earlier + rise[...] * later
        if len(blocks) == 2:
            fields[pl.ds(6 * BLOCK, 8), :] = stats[...]


def join_kernel(digit, own, came, packet):
    own, came = unpacked(own[...]), unpacked(came[...])
    second = my_place()[digit] == 1
    packet[...] = packed(*joined(chosen(second, came, own), chosen(second, own, came)))


def entering_kernel(pair, came_0, came_1, came_2, neighbour, entering):
    z, y_lo, _ = my_place()
    packets = [pair[...]] + [ref[...] for ref in (came_0, came_1, came_2)]
    sources = [z]
    for sends in Z_ROUND:
        source = sends.index(3)
        for k in range(3):
            source = jnp.where(z == k, sends.index(k), source)
        sources.append(source)
    before = jnp.zeros((8, LANES), jnp.float32)
    after = before
    ordered = []
    for k in range(4):
        packet = packets[0]
        for source, other in zip(sources[1:], packets[1:]):
            packet = jnp.where(source == k, other, packet)
        ordered.append(unpacked(packet))
    for k in range(4):
        keep, forward, _ = ordered[k]
        before = jnp.where(k < z, keep * before + forward, before)
        keep, _, backward = ordered[3 - k]
        after = jnp.where(3 - k > z, keep * after + backward, after)
    keep, forward, backward = unpacked(neighbour[...])
    before = jnp.where(y_lo == 1, keep * before + forward, before)
    after = jnp.where(y_lo == 0, keep * after + backward, after)
    entering[...] = jnp.concatenate([before, after], axis=0)


def entering_blocks(before, after, stats):
    before, after = wide(before), wide(after)
    keep_0, forward_0, keep_1, backward_1 = (stats[k : k + 1, :] for k in range(4))
    return (before, keep_0 * (keep_1 * after + backward_1)), (keep_0 * before + forward_0, keep_1 * after)


def filtered(fields, entering, use):
    for k in range(2 * BLOCK // 8):
        block, row = divmod(8 * k, BLOCK)
        local, fall, rise = (field(fields, block, j)[pl.ds(row, 8), :] for j in range(3))
        first, second = entering[block]
        use(k, local + fall * first + rise * second)


def power_kernel(entering, own, partner, fields, stats, gain, fields_0, states, power_out):
    core = my_place()[2]

    @pl.when(core == 0)
    def _():
        power_out[...] = jnp.zeros((8, LANES), jnp.float32)

    @pl.when(core == 1)
    def _():
        before, after = entering[:8], entering[8:]
        lane = lax.broadcasted_iota(jnp.int32, (8, LANES), 1)
        power = [jnp.zeros((8, LANES), jnp.float32)]
        scale = gain[...]

        def add(place, state):
            square = functools.reduce(jnp.add, rows_of(state * state))
            power[0] = jnp.where(lane == place, jnp.sum(square, axis=1, keepdims=True), power[0])

        def keep_it(k, state):
            states[pl.ds(8 * k, 8), :] = state * scale
            add(LANES // 2 + k, state)

        keep, forward, _ = unpacked(partner[...])
        filtered(fields, entering_blocks(keep * before + forward, after, stats), keep_it)
        keep, _, backward = unpacked(own[...])
        stats_0 = fields_0[pl.ds(6 * BLOCK, 8), :]
        filtered(fields_0, entering_blocks(before, keep * after + backward, stats_0), add)
        power_out[...] = power[0]


def states_kernel(came, partner, fields, stats, gain, states_1, states):
    @pl.when(my_place()[2] == 0)
    def _():
        before, after = came[:8], came[8:]
        keep, _, backward = unpacked(partner[...])
        scale = gain[...]

        def keep_it(k, state):
            states[pl.ds(8 * k, 8), :] = state * scale

        filtered(fields, entering_blocks(before, keep * after + backward, stats), keep_it)


def norm_kernel(mine, scale, channels, power, states, *refs):
    mixed_hbm, mixed, left = refs[-3:]

    @pl.when(my_place()[2] == mine)
    def _():
        factor = lax.rsqrt(power[...] * (scale * scale / channels) + 1e-6) * scale
        pieces = left.shape[0]
        height = states.shape[0] // pieces
        copies = []
        for piece in range(pieces):
            for k in range(piece * height // 16, (piece + 1) * height // 16):
                halves = []
                for j in (2 * k, 2 * k + 1):
                    place = j + mine * (LANES // 2)
                    halves.append(states[pl.ds(8 * j, 8), :] * factor[:, place : place + 1])
                mixed[pl.ds(16 * k, 16), :] = jnp.concatenate(halves, axis=0).astype(jnp.bfloat16)
            span = pl.ds(piece * height, height)
            copy = pltpu.make_async_copy(mixed.at[span], mixed_hbm.at[span], left.at[piece])
            copy.start()
            copies.append(copy)
        for copy in copies:
            copy.wait()


VMEM = pl.BlockSpec(memory_space=pltpu.VMEM)
HBM = pl.BlockSpec(memory_space=pltpu.HBM)
PARAMS = pltpu.CompilerParams(vmem_limit_bytes=16 << 20)
SPACES = ("time", "chan")


def placed(space, *arrays):
    return [pltpu.with_memory_space_constraint(array, space) for array in arrays]


def call(kernel, outs, *arrays, scratch=(), aliases={}):
    return pl.pallas_call(
        kernel,
        out_shape=tuple(outs),
        in_specs=[VMEM] * len(arrays),
        out_specs=(VMEM,) * len(outs),
        scratch_shapes=scratch,
        input_output_aliases=aliases,
        compiler_params=PARAMS,
    )(*placed(pltpu.VMEM, *arrays))


def moved(value, target):
    pairs = []
    for place in range(128):
        t, c = place // 8, place % 8
        z, y_lo, core, y_hi, x = target(t // 4, (t // 2) % 2, t % 2, c // 4, c % 4)
        pairs.append((place, (z * 4 + y_lo * 2 + core) * 8 + y_hi * 4 + x))
    return lax.ppermute(value, SPACES, pairs)


def between_cores(value):
    return moved(
        value, lambda z, y_lo, core, y_hi, x: (z, y_lo, 1 - core, y_hi, x))


def relayed(value, target):
    return moved(
        value,
        lambda z, y_lo, core, y_hi, x: (
            (*target(z, y_lo, y_hi, x)[:2], 1, *target(z, y_lo, y_hi, x)[2:]) if core else (z, 1 - y_lo, 0, y_hi, x)
        ),
    )


def per_device(fade_rate, update_in, norm_gain):
    time, chan = lax.axis_size("time"), lax.axis_size("chan")
    length, width = fade_rate.shape[1:]
    total_length = length * time
    per_rate = math.log2(math.e) / total_length
    full = pltpu.VMEM((length, width), jnp.float32)
    packet = pltpu.VMEM((16, LANES), jnp.float32)
    tile = pltpu.VMEM((8, LANES), jnp.float32)
    rate, spent, push, stats, own, gain = pl.pallas_call(
        functools.partial(ends_kernel, per_rate),
        out_shape=(
            full,
            full,
            pltpu.VMEM((length, width), jnp.bfloat16),
            pltpu.VMEM((8, width), jnp.float32),
            packet,
            pltpu.VMEM((1, width), jnp.float32),
        ),
        in_specs=[HBM] * 3,
        out_specs=(VMEM,) * 6,
        scratch_shapes=[pltpu.SemaphoreType.DMA((2, length // BLOCK + 1))],
        compiler_params=PARAMS,
        name="ends",
    )(*placed(pltpu.HBM, fade_rate[0], update_in[0], norm_gain[None]))

    def local(mine, blocks, *others):
        half = pltpu.VMEM((BLOCK, width), jnp.bfloat16)
        return call(
            functools.partial(local_kernel, mine, blocks, per_rate),
            [pltpu.VMEM((6 * BLOCK + 8, width), jnp.float32)],
            rate,
            spent,
            push,
            stats,
            *others,
            scratch=[half, half],
            aliases={4: 0} if others else {},
        )[0]

    fields_0 = local(0, (0, 1))
    fields = local(1, (1,), local(1, (0,)))
    partner = between_cores(own)
    (chip,) = call(functools.partial(join_kernel, 2), [packet], own, partner)
    neighbour = relayed(chip, lambda z, y_lo, y_hi, x: (z, 1 - y_lo, y_hi, x))
    (pair,) = call(functools.partial(join_kernel, 1), [packet], chip, neighbour)
    around = [relayed(pair, lambda z, y_lo, y_hi, x, to=to: (to[z], y_lo, y_hi, x)) for to in Z_ROUND]
    (entering,) = call(entering_kernel, [packet], pair, *around, neighbour)
    sent = between_cores(fields_0)
    came = between_cores(entering)
    states, power = call(power_kernel, [full, tile], entering, own, partner, fields, stats, gain, sent)
    (states,) = call(states_kernel, [full], came, partner, fields_0, stats, gain, states, aliases={5: 0})

    power = power + relayed(power, lambda z, y_lo, y_hi, x: (z, y_lo, 1 - y_hi, x))
    for part in [relayed(power, lambda z, y_lo, y_hi, x, to=to: (z, y_lo, y_hi, to[x])) for to in X_ROUND]:
        power = power + part
    came = between_cores(power)

    def norm(mine, power, *before):
        return pl.pallas_call(
            functools.partial(norm_kernel, mine, float(total_length) ** -0.5, width * chan),
            out_shape=jax.ShapeDtypeStruct((length, width), jnp.bfloat16),
            in_specs=[VMEM] * 2 + [HBM] * len(before),
            out_specs=HBM,
            input_output_aliases={2: 0} if before else {},
            scratch_shapes=[pltpu.VMEM((length, width), jnp.bfloat16), pltpu.SemaphoreType.DMA((4,))],
            compiler_params=PARAMS,
        )(*placed(pltpu.VMEM, power, states), *placed(pltpu.HBM, *before))

    return norm(0, came, norm(1, power))[None]


def solution(mesh):
    shard = P(None, "time", "chan")
    return jax.shard_map(per_device, mesh=mesh, in_specs=(shard, shard, P("chan")), out_specs=shard, check_vma=False)
```

```python
import functools
import math

import jax
import jax.numpy as jnp
from jax import lax
from jax.experimental import pallas as pl
from jax.experimental.pallas import tpu as pltpu
from jax.sharding import PartitionSpec as P


LANES = 128
BLOCK = 256
Z_ROUND = ((1, 3, 0, 2), (3, 2, 1, 0), (2, 0, 3, 1))
X_ROUND = ((1, 3, 0, 2), (3, 2, 1, 0), (2, 0, 3, 1))


def dot(a, b):
    return jnp.dot(a, b, preferred_element_type=jnp.float32)


def rows_of(row):
    return [row[:, k : k + LANES] for k in range(0, row.shape[1], LANES)]


def triangle(keeps):
    shape = (BLOCK, BLOCK)
    kept = keeps(lax.broadcasted_iota(jnp.int32, shape, 0), lax.broadcasted_iota(jnp.int32, shape, 1))
    return jnp.where(kept, 1.0, 0.0).astype(jnp.bfloat16)


def wide(tile):
    return jnp.concatenate([tile[k : k + 1] for k in range(4)], axis=1)


def my_place():
    me = lax.axis_index("time")
    return me // 4, (me // 2) % 2, me % 2


def unpacked(packet):
    first, second = packet[:8], packet[8:]
    return first, pltpu.roll(first, 4, axis=0), second


def packed(keep, forward, backward):
    return jnp.concatenate([keep[:4], forward[:4], backward[:4], keep[:4]], axis=0)


def joined(earlier, later):
    keep_0, forward_0, backward_0 = earlier
    keep_1, forward_1, backward_1 = later
    return keep_0 * keep_1, keep_1 * forward_0 + forward_1, backward_0 + keep_0 * backward_1


def chosen(take, yes, no):
    return tuple(jnp.where(take, a, b) for a, b in zip(yes, no))


def ends_kernel(per_rate, rate_hbm, update_hbm, gain_hbm, rate, spent, push, stats, packet, gain, arrived):
    blocks = rate.shape[0] // BLOCK
    copies = []
    for k in range(blocks):
        span = pl.ds(k * BLOCK, BLOCK)
        copies.append(pltpu.make_async_copy(rate_hbm.at[span], rate.at[span], arrived.at[0, k]))
        copies.append(pltpu.make_async_copy(update_hbm.at[span], push.at[span], arrived.at[1, k]))
    copies.append(pltpu.make_async_copy(gain_hbm, gain, arrived.at[0, blocks]))
    for copy in copies:
        copy.start()
    half = BLOCK // 2
    line = lax.broadcasted_iota(jnp.int32, (half, BLOCK), 0)
    column = lax.broadcasted_iota(jnp.int32, (half, BLOCK), 1) % half
    twice_lower = jnp.where(line >= column, 1.0, 0.0).astype(jnp.bfloat16)
    ends = []
    for k in range(blocks):
        copies[2 * k].wait()
        so_far = 0.0
        for row in range(k * BLOCK, (k + 1) * BLOCK, half):
            span = pl.ds(row, half)
            step = rate[span, :] * per_rate
            high = step.astype(jnp.bfloat16)
            low = (step - high.astype(jnp.float32)).astype(jnp.bfloat16)
            spent[span, :] = dot(twice_lower, jnp.concatenate([high, low], axis=0)) + so_far
            so_far = spent[pl.ds(row + half - 8, 8), :][7:]
        copies[2 * k + 1].wait()
        forward = jnp.zeros((8, rate.shape[1]), jnp.float32)
        backward = forward
        for row in range(k * BLOCK, (k + 1) * BLOCK, 16):
            rows = pl.ds(row, 16)
            total = spent[rows, :]
            update = push[rows, :].astype(jnp.float32)
            more = jnp.exp2(total) * update
            less = jnp.exp2(rate[rows, :] * per_rate - total) * update
            forward = forward + (more[:8] + more[8:])
            backward = backward + (less[:8] + less[8:])
        keep = jnp.exp2(-spent[pl.ds((k + 1) * BLOCK - 8, 8), :][7:])
        ends.append((keep, keep * jnp.sum(forward, axis=0, keepdims=True), jnp.sum(backward, axis=0, keepdims=True)))
    keep, forward, backward = joined(*ends)
    copies[-1].wait()
    row = ends[0][0]
    stats[...] = jnp.concatenate([ends[0][0], ends[0][1], ends[1][0], ends[1][2], row, row, row, row], axis=0)
    packet[...] = jnp.concatenate(rows_of(keep) + rows_of(forward) + rows_of(backward) + rows_of(keep), axis=0)


def field(fields, block, k):
    return fields.at[pl.ds((3 * block + k) * BLOCK, BLOCK)]


def local_kernel(mine, blocks, per_rate, rate, spent, push, stats, *refs):
    fields, ahead, behind = refs[-3:]

    @pl.when(my_place()[2] == mine)
    def _():
        lower, upper = triangle(jnp.greater_equal), triangle(jnp.less_equal)
        for block in blocks:
            local, fall, rise = (field(fields, block, k) for k in range(3))
            for row in range(0, BLOCK, 16):
                rows, here = pl.ds(block * BLOCK + row, 16), pl.ds(row, 16)
                total = spent[rows, :]
                before = total - rate[rows, :] * per_rate
                update = push[rows, :].astype(jnp.float32)
                fall[here, :] = jnp.exp2(-total)
                rise[here, :] = jnp.exp2(before)
                ahead[here, :] = ((jnp.exp2(total) - 1.0) * update).astype(jnp.bfloat16)
                behind[here, :] = ((jnp.exp2(-before) - 1.0) * update).astype(jnp.bfloat16)
            update = push[pl.ds(block * BLOCK, BLOCK), :]
            earlier = dot(lower, update) + dot(lower, ahead[...])
            later = dot(upper, update) + dot(upper, behind[...])
            local[...] = fall[...] * earlier + rise[...] * later
        if len(blocks) == 2:
            fields[pl.ds(6 * BLOCK, 8), :] = stats[...]


def table(values, place):
    chosen_value = jnp.int32(values[-1])
    for k, value in enumerate(values[:-1]):
        chosen_value = jnp.where(place == k, value, chosen_value)
    return chosen_value


def pair_kernel(own, partner, other_1, other_0, neighbour, *sends):
    z, y_lo, _ = my_place()
    chip = joined(unpacked(partner[...]), unpacked(own[...]))
    other = joined(unpacked(other_0[...]), unpacked(other_1[...]))
    neighbour[...] = packed(*other)
    second = y_lo == 1
    keep, forward, backward = joined(chosen(second, other, chip), chosen(second, chip, other))
    for places, send in zip(Z_ROUND, sends):
        send[...] = jnp.concatenate([keep[:4], jnp.where(table(places, z) > z, forward, backward)[:4]], axis=0)


def entering_kernel(came_0, came_1, came_2, neighbour, entering):
    z, y_lo, _ = my_place()
    packets = [ref[...] for ref in (came_0, came_1, came_2)]
    sources = [table([places.index(k) for k in range(4)], z) for places in Z_ROUND]
    before = jnp.zeros((8, LANES), jnp.float32)
    after = before
    ordered = []
    for k in range(4):
        packet = packets[0]
        for source, other in zip(sources[1:], packets[1:]):
            packet = jnp.where(source == k, other, packet)
        ordered.append((packet, pltpu.roll(packet, 4, axis=0)))
    for k in range(4):
        keep, forward = ordered[k]
        before = jnp.where(k < z, keep * before + forward, before)
        keep, backward = ordered[3 - k]
        after = jnp.where(3 - k > z, keep * after + backward, after)
    keep, forward, backward = unpacked(neighbour[...])
    before = jnp.where(y_lo == 1, keep * before + forward, before)
    after = jnp.where(y_lo == 0, keep * after + backward, after)
    entering[...] = jnp.concatenate([before, after], axis=0)


def entering_blocks(before, after, stats):
    before, after = wide(before), wide(after)
    keep_0, forward_0, keep_1, backward_1 = (stats[k : k + 1, :] for k in range(4))
    return (before, keep_0 * (keep_1 * after + backward_1)), (keep_0 * before + forward_0, keep_1 * after)


def filtered(fields, entering, use):
    for k in range(2 * BLOCK // 8):
        block, row = divmod(8 * k, BLOCK)
        local, fall, rise = (field(fields, block, j)[pl.ds(row, 8), :] for j in range(3))
        first, second = entering[block]
        use(k, local + fall * first + rise * second)


def power_kernel(entering, own, partner, fields, stats, fields_0, states, power_out):
    core = my_place()[2]

    @pl.when(core == 0)
    def _():
        power_out[...] = jnp.zeros((8, LANES), jnp.float32)

    @pl.when(core == 1)
    def _():
        before, after = entering[:8], entering[8:]
        lane = lax.broadcasted_iota(jnp.int32, (8, LANES), 1)
        power = [jnp.zeros((8, LANES), jnp.float32)]

        def add(place, state):
            square = functools.reduce(jnp.add, rows_of(state * state))
            power[0] = jnp.where(lane == place, jnp.sum(square, axis=1, keepdims=True), power[0])

        def keep_it(k, state):
            states[pl.ds(8 * k, 8), :] = state
            add(LANES // 2 + k, state)

        keep, forward, _ = unpacked(partner[...])
        filtered(fields, entering_blocks(keep * before + forward, after, stats), keep_it)
        keep, _, backward = unpacked(own[...])
        stats_0 = fields_0[pl.ds(6 * BLOCK, 8), :]
        filtered(fields_0, entering_blocks(before, keep * after + backward, stats_0), add)
        power_out[...] = power[0]


def states_kernel(came, partner, fields, stats, gain, states_1, states):
    @pl.when(my_place()[2] == 0)
    def _():
        before, after = came[:8], came[8:]
        keep, _, backward = unpacked(partner[...])
        scale = gain[...]

        def keep_it(k, state):
            states[pl.ds(8 * k, 8), :] = state * scale

        filtered(fields, entering_blocks(before, keep * after + backward, stats), keep_it)


def norm_kernel(mine, scale, channels, power, states, gain, *refs):
    mixed_hbm, mixed, left = refs[-3:]

    @pl.when(my_place()[2] == mine)
    def _():
        factor = lax.rsqrt(power[...] * (scale * scale / channels) + 1e-6) * scale
        gains = gain[...]
        pieces = left.shape[0]
        height = states.shape[0] // pieces
        copies = []
        for piece in range(pieces):
            for k in range(piece * height // 16, (piece + 1) * height // 16):
                halves = []
                for j in (2 * k, 2 * k + 1):
                    place = j + mine * (LANES // 2)
                    half = states[pl.ds(8 * j, 8), :] * factor[:, place : place + 1]
                    halves.append(half * gains if mine else half)
                mixed[pl.ds(16 * k, 16), :] = jnp.concatenate(halves, axis=0).astype(jnp.bfloat16)
            span = pl.ds(piece * height, height)
            copy = pltpu.make_async_copy(mixed.at[span], mixed_hbm.at[span], left.at[piece])
            copy.start()
            copies.append(copy)
        for copy in copies:
            copy.wait()


VMEM = pl.BlockSpec(memory_space=pltpu.VMEM)
HBM = pl.BlockSpec(memory_space=pltpu.HBM)
PARAMS = pltpu.CompilerParams(vmem_limit_bytes=16 << 20)
SPACES = ("time", "chan")


def placed(space, *arrays):
    return [pltpu.with_memory_space_constraint(array, space) for array in arrays]


def call(kernel, outs, *arrays, scratch=(), aliases={}):
    return pl.pallas_call(
        kernel,
        out_shape=tuple(outs),
        in_specs=[VMEM] * len(arrays),
        out_specs=(VMEM,) * len(outs),
        scratch_shapes=scratch,
        input_output_aliases=aliases,
        compiler_params=PARAMS,
    )(*placed(pltpu.VMEM, *arrays))


def moved(value, target):
    pairs = []
    for place in range(128):
        t, c = place // 8, place % 8
        z, y_lo, core, y_hi, x = target(t // 4, (t // 2) % 2, t % 2, c // 4, c % 4)
        pairs.append((place, (z * 4 + y_lo * 2 + core) * 8 + y_hi * 4 + x))
    return lax.ppermute(value, SPACES, pairs)


def between_cores(value):
    return moved(
        value, lambda z, y_lo, core, y_hi, x: (z, y_lo, 1 - core, y_hi, x))


def relayed(value, target):
    return moved(
        value,
        lambda z, y_lo, core, y_hi, x: (
            (*target(z, y_lo, y_hi, x)[:2], 1, *target(z, y_lo, y_hi, x)[2:]) if core else (z, 1 - y_lo, 0, y_hi, x)
        ),
    )


def per_device(fade_rate, update_in, norm_gain):
    time, chan = lax.axis_size("time"), lax.axis_size("chan")
    length, width = fade_rate.shape[1:]
    total_length = length * time
    per_rate = math.log2(math.e) / total_length
    full = pltpu.VMEM((length, width), jnp.float32)
    packet = pltpu.VMEM((16, LANES), jnp.float32)
    tile = pltpu.VMEM((8, LANES), jnp.float32)
    rate, spent, push, stats, own, gain = pl.pallas_call(
        functools.partial(ends_kernel, per_rate),
        out_shape=(
            full,
            full,
            pltpu.VMEM((length, width), jnp.bfloat16),
            pltpu.VMEM((8, width), jnp.float32),
            packet,
            pltpu.VMEM((1, width), jnp.float32),
        ),
        in_specs=[HBM] * 3,
        out_specs=(VMEM,) * 6,
        scratch_shapes=[pltpu.SemaphoreType.DMA((2, length // BLOCK + 1))],
        compiler_params=PARAMS,
        name="ends",
    )(*placed(pltpu.HBM, fade_rate[0], update_in[0], norm_gain[None]))

    def local(mine, blocks, *others):
        half = pltpu.VMEM((BLOCK, width), jnp.bfloat16)
        return call(
            functools.partial(local_kernel, mine, blocks, per_rate),
            [pltpu.VMEM((6 * BLOCK + 8, width), jnp.float32)],
            rate,
            spent,
            push,
            stats,
            *others,
            scratch=[half, half],
            aliases={4: 0} if others else {},
        )[0]

    fields_0 = local(0, (0, 1))
    fields = local(1, (1,), local(1, (0,)))
    other_0 = moved(own, lambda z, y_lo, core, y_hi, x: (z, y_lo if core else 1 - y_lo, 1 - core, y_hi, x))
    other_1 = moved(own, lambda z, y_lo, core, y_hi, x: (z, 1 - y_lo, core, y_hi, x))
    partner = between_cores(own)
    neighbour, *sends = call(pair_kernel, [packet, tile, tile, tile], own, partner, other_1, other_0)
    around = [relayed(send, lambda z, y_lo, y_hi, x, to=to: (to[z], y_lo, y_hi, x)) for send, to in zip(sends, Z_ROUND)]
    (entering,) = call(entering_kernel, [packet], *around, neighbour)
    sent = between_cores(fields_0)
    came = between_cores(entering)
    states, power = call(power_kernel, [full, tile], entering, own, partner, fields, stats, sent)
    (states,) = call(states_kernel, [full], came, partner, fields_0, stats, gain, states, aliases={5: 0})

    power = power + relayed(power, lambda z, y_lo, y_hi, x: (z, y_lo, 1 - y_hi, x))
    for part in [relayed(power, lambda z, y_lo, y_hi, x, to=to: (z, y_lo, y_hi, to[x])) for to in X_ROUND]:
        power = power + part
    came = between_cores(power)

    def norm(mine, power, *before):
        return pl.pallas_call(
            functools.partial(norm_kernel, mine, float(total_length) ** -0.5, width * chan),
            out_shape=jax.ShapeDtypeStruct((length, width), jnp.bfloat16),
            in_specs=[VMEM] * 3 + [HBM] * len(before),
            out_specs=HBM,
            input_output_aliases={3: 0} if before else {},
            scratch_shapes=[pltpu.VMEM((length, width), jnp.bfloat16), pltpu.SemaphoreType.DMA((4,))],
            compiler_params=PARAMS,
        )(*placed(pltpu.VMEM, power, states, gain), *placed(pltpu.HBM, *before))

    return norm(0, came, norm(1, power))[None]


def solution(mesh):
    shard = P(None, "time", "chan")
    return jax.shard_map(per_device, mesh=mesh, in_specs=(shard, shard, P("chan")), out_specs=shard, check_vma=False)
```

```python
import functools
import math

import jax
import jax.numpy as jnp
from jax import lax
from jax.experimental import pallas as pl
from jax.experimental.pallas import tpu as pltpu
from jax.sharding import PartitionSpec as P


LANES = 128
BLOCK = 256
Z_ROUND = ((1, 3, 0, 2), (3, 2, 1, 0), (2, 0, 3, 1))
X_ROUND = ((1, 3, 0, 2), (3, 2, 1, 0), (2, 0, 3, 1))


def dot(a, b):
    return jnp.dot(a, b, preferred_element_type=jnp.float32)


def rows_of(row):
    return [row[:, k : k + LANES] for k in range(0, row.shape[1], LANES)]


def triangle(keeps):
    shape = (BLOCK, BLOCK)
    kept = keeps(lax.broadcasted_iota(jnp.int32, shape, 0), lax.broadcasted_iota(jnp.int32, shape, 1))
    return jnp.where(kept, 1.0, 0.0).astype(jnp.bfloat16)


def wide(tile):
    return jnp.concatenate([tile[k : k + 1] for k in range(4)], axis=1)


def my_place():
    me = lax.axis_index("time")
    return me // 4, (me // 2) % 2, me % 2


def unpacked(packet):
    first, second = packet[:8], packet[8:]
    return first, pltpu.roll(first, 4, axis=0), second


def packed(keep, forward, backward):
    return jnp.concatenate([keep[:4], forward[:4], backward[:4], keep[:4]], axis=0)


def joined(earlier, later):
    keep_0, forward_0, backward_0 = earlier
    keep_1, forward_1, backward_1 = later
    return keep_0 * keep_1, keep_1 * forward_0 + forward_1, backward_0 + keep_0 * backward_1


def chosen(take, yes, no):
    return tuple(jnp.where(take, a, b) for a, b in zip(yes, no))


def ends_kernel(per_rate, rate_hbm, update_hbm, gain_hbm, earlier, spent, push, stats, packet, gain, rate, arrived):
    blocks = rate.shape[0] // BLOCK
    copies = []
    for k in range(blocks):
        span = pl.ds(k * BLOCK, BLOCK)
        copies.append(pltpu.make_async_copy(rate_hbm.at[span], rate.at[span], arrived.at[0, k]))
        copies.append(pltpu.make_async_copy(update_hbm.at[span], push.at[span], arrived.at[1, k]))
    copies.append(pltpu.make_async_copy(gain_hbm, gain, arrived.at[0, blocks]))
    for copy in copies:
        copy.start()
    half = BLOCK // 2
    line = lax.broadcasted_iota(jnp.int32, (half, BLOCK), 0)
    column = lax.broadcasted_iota(jnp.int32, (half, BLOCK), 1) % half
    twice_lower = jnp.where(line >= column, 1.0, 0.0).astype(jnp.bfloat16)
    ends = []
    for k in range(blocks):
        copies[2 * k].wait()
        so_far = 0.0
        for row in range(k * BLOCK, (k + 1) * BLOCK, half):
            span = pl.ds(row, half)
            step = rate[span, :] * per_rate
            high = step.astype(jnp.bfloat16)
            low = (step - high.astype(jnp.float32)).astype(jnp.bfloat16)
            total = dot(twice_lower, jnp.concatenate([high, low], axis=0)) + so_far
            spent[span, :] = total
            earlier[span, :] = total - rate[span, :] * per_rate
            so_far = spent[pl.ds(row + half - 8, 8), :][7:]
        copies[2 * k + 1].wait()
        forward = jnp.zeros((8, rate.shape[1]), jnp.float32)
        backward = forward
        for row in range(k * BLOCK, (k + 1) * BLOCK, 16):
            rows = pl.ds(row, 16)
            total = spent[rows, :]
            update = push[rows, :].astype(jnp.float32)
            more = jnp.exp2(total) * update
            less = jnp.exp2(-earlier[rows, :]) * update
            forward = forward + (more[:8] + more[8:])
            backward = backward + (less[:8] + less[8:])
        keep = jnp.exp2(-spent[pl.ds((k + 1) * BLOCK - 8, 8), :][7:])
        ends.append((keep, keep * jnp.sum(forward, axis=0, keepdims=True), jnp.sum(backward, axis=0, keepdims=True)))
    keep, forward, backward = joined(*ends)
    copies[-1].wait()
    row = ends[0][0]
    stats[...] = jnp.concatenate([ends[0][0], ends[0][1], ends[1][0], ends[1][2], row, row, row, row], axis=0)
    packet[...] = jnp.concatenate(rows_of(keep) + rows_of(forward) + rows_of(backward) + rows_of(keep), axis=0)


def field(fields, block, k):
    return fields.at[pl.ds((3 * block + k) * BLOCK, BLOCK)]


def local_kernel(mine, blocks, earlier, spent, push, stats, *refs):
    fields, ahead, behind = refs[-3:]

    @pl.when(my_place()[2] == mine)
    def _():
        lower, upper = triangle(jnp.greater_equal), triangle(jnp.less_equal)
        for block in blocks:
            local, fall, rise = (field(fields, block, k) for k in range(3))
            for row in range(0, BLOCK, 16):
                rows, here = pl.ds(block * BLOCK + row, 16), pl.ds(row, 16)
                total = spent[rows, :]
                before = earlier[rows, :]
                update = push[rows, :].astype(jnp.float32)
                fall[here, :] = jnp.exp2(-total)
                rise[here, :] = jnp.exp2(before)
                ahead[here, :] = ((jnp.exp2(total) - 1.0) * update).astype(jnp.bfloat16)
                behind[here, :] = ((jnp.exp2(-before) - 1.0) * update).astype(jnp.bfloat16)
            update = push[pl.ds(block * BLOCK, BLOCK), :]
            sums = dot(lower, update) + dot(lower, ahead[...])
            later = dot(upper, update) + dot(upper, behind[...])
            local[...] = fall[...] * sums + rise[...] * later
        if len(blocks) == 2:
            fields[pl.ds(6 * BLOCK, 8), :] = stats[...]


def table(values, place):
    chosen_value = jnp.int32(values[-1])
    for k, value in enumerate(values[:-1]):
        chosen_value = jnp.where(place == k, value, chosen_value)
    return chosen_value


def pair_kernel(own, partner, other_1, other_0, neighbour, *sends):
    z, y_lo, _ = my_place()
    chip = joined(unpacked(partner[...]), unpacked(own[...]))
    other = joined(unpacked(other_0[...]), unpacked(other_1[...]))
    neighbour[...] = packed(*other)
    second = y_lo == 1
    keep, forward, backward = joined(chosen(second, other, chip), chosen(second, chip, other))
    for places, send in zip(Z_ROUND, sends):
        send[...] = jnp.concatenate([keep[:4], jnp.where(table(places, z) > z, forward, backward)[:4]], axis=0)


def entering_kernel(came_0, came_1, came_2, neighbour, entering):
    z, y_lo, _ = my_place()
    packets = [ref[...] for ref in (came_0, came_1, came_2)]
    sources = [table([places.index(k) for k in range(4)], z) for places in Z_ROUND]
    before = jnp.zeros((8, LANES), jnp.float32)
    after = before
    ordered = []
    for k in range(4):
        packet = packets[0]
        for source, other in zip(sources[1:], packets[1:]):
            packet = jnp.where(source == k, other, packet)
        ordered.append((packet, pltpu.roll(packet, 4, axis=0)))
    for k in range(4):
        keep, forward = ordered[k]
        before = jnp.where(k < z, keep * before + forward, before)
        keep, backward = ordered[3 - k]
        after = jnp.where(3 - k > z, keep * after + backward, after)
    keep, forward, backward = unpacked(neighbour[...])
    before = jnp.where(y_lo == 1, keep * before + forward, before)
    after = jnp.where(y_lo == 0, keep * after + backward, after)
    entering[...] = jnp.concatenate([before, after], axis=0)


def entering_blocks(before, after, stats):
    before, after = wide(before), wide(after)
    keep_0, forward_0, keep_1, backward_1 = (stats[k : k + 1, :] for k in range(4))
    return (before, keep_0 * (keep_1 * after + backward_1)), (keep_0 * before + forward_0, keep_1 * after)


def filtered(fields, entering, use):
    for k in range(2 * BLOCK // 8):
        block, row = divmod(8 * k, BLOCK)
        local, fall, rise = (field(fields, block, j)[pl.ds(row, 8), :] for j in range(3))
        first, second = entering[block]
        use(k, local + fall * first + rise * second)


def power_kernel(entering, own, partner, fields, stats, fields_0, states, power_out):
    core = my_place()[2]

    @pl.when(core == 0)
    def _():
        power_out[...] = jnp.zeros((8, LANES), jnp.float32)

    @pl.when(core == 1)
    def _():
        before, after = entering[:8], entering[8:]
        lane = lax.broadcasted_iota(jnp.int32, (8, LANES), 1)
        power = [jnp.zeros((8, LANES), jnp.float32)] * 4

        def add(place, state):
            square = functools.reduce(jnp.add, rows_of(state * state))
            power[place % 4] = jnp.where(lane == place, jnp.sum(square, axis=1, keepdims=True), power[place % 4])

        def keep_it(k, state):
            states[pl.ds(8 * k, 8), :] = state
            add(LANES // 2 + k, state)

        keep, forward, _ = unpacked(partner[...])
        filtered(fields, entering_blocks(keep * before + forward, after, stats), keep_it)
        keep, _, backward = unpacked(own[...])
        stats_0 = fields_0[pl.ds(6 * BLOCK, 8), :]
        filtered(fields_0, entering_blocks(before, keep * after + backward, stats_0), add)
        power_out[...] = (power[0] + power[1]) + (power[2] + power[3])


def states_kernel(came, partner, fields, stats, gain, states_1, states):
    @pl.when(my_place()[2] == 0)
    def _():
        before, after = came[:8], came[8:]
        keep, _, backward = unpacked(partner[...])
        scale = gain[...]

        def keep_it(k, state):
            states[pl.ds(8 * k, 8), :] = state * scale

        filtered(fields, entering_blocks(before, keep * after + backward, stats), keep_it)


def norm_kernel(mine, scale, channels, power, states, gain, *refs):
    mixed_hbm, mixed, left = refs[-3:]

    @pl.when(my_place()[2] == mine)
    def _():
        factor = lax.rsqrt(power[...] * (scale * scale / channels) + 1e-6) * scale
        gains = gain[...]
        pieces = left.shape[0]
        height = states.shape[0] // pieces
        copies = []
        for piece in range(pieces):
            for k in range(piece * height // 16, (piece + 1) * height // 16):
                halves = []
                for j in (2 * k, 2 * k + 1):
                    place = j + mine * (LANES // 2)
                    half = states[pl.ds(8 * j, 8), :] * factor[:, place : place + 1]
                    halves.append(half * gains if mine else half)
                mixed[pl.ds(16 * k, 16), :] = jnp.concatenate(halves, axis=0).astype(jnp.bfloat16)
            span = pl.ds(piece * height, height)
            copy = pltpu.make_async_copy(mixed.at[span], mixed_hbm.at[span], left.at[piece])
            copy.start()
            copies.append(copy)
        for copy in copies:
            copy.wait()


VMEM = pl.BlockSpec(memory_space=pltpu.VMEM)
HBM = pl.BlockSpec(memory_space=pltpu.HBM)
PARAMS = pltpu.CompilerParams(vmem_limit_bytes=16 << 20)
SPACES = ("time", "chan")


def placed(space, *arrays):
    return [pltpu.with_memory_space_constraint(array, space) for array in arrays]


def call(kernel, outs, *arrays, scratch=(), aliases={}):
    return pl.pallas_call(
        kernel,
        out_shape=tuple(outs),
        in_specs=[VMEM] * len(arrays),
        out_specs=(VMEM,) * len(outs),
        scratch_shapes=scratch,
        input_output_aliases=aliases,
        compiler_params=PARAMS,
    )(*placed(pltpu.VMEM, *arrays))


def moved(value, target):
    pairs = []
    for place in range(128):
        t, c = place // 8, place % 8
        z, y_lo, core, y_hi, x = target(t // 4, (t // 2) % 2, t % 2, c // 4, c % 4)
        pairs.append((place, (z * 4 + y_lo * 2 + core) * 8 + y_hi * 4 + x))
    return lax.ppermute(value, SPACES, pairs)


def between_cores(value):
    return moved(
        value, lambda z, y_lo, core, y_hi, x: (z, y_lo, 1 - core, y_hi, x))


def relayed(value, target):
    return moved(
        value,
        lambda z, y_lo, core, y_hi, x: (
            (*target(z, y_lo, y_hi, x)[:2], 1, *target(z, y_lo, y_hi, x)[2:]) if core else (z, 1 - y_lo, 0, y_hi, x)
        ),
    )


def per_device(fade_rate, update_in, norm_gain):
    time, chan = lax.axis_size("time"), lax.axis_size("chan")
    length, width = fade_rate.shape[1:]
    total_length = length * time
    per_rate = math.log2(math.e) / total_length
    full = pltpu.VMEM((length, width), jnp.float32)
    packet = pltpu.VMEM((16, LANES), jnp.float32)
    tile = pltpu.VMEM((8, LANES), jnp.float32)
    earlier, spent, push, stats, own, gain = pl.pallas_call(
        functools.partial(ends_kernel, per_rate),
        out_shape=(
            full,
            full,
            pltpu.VMEM((length, width), jnp.bfloat16),
            pltpu.VMEM((8, width), jnp.float32),
            packet,
            pltpu.VMEM((1, width), jnp.float32),
        ),
        in_specs=[HBM] * 3,
        out_specs=(VMEM,) * 6,
        scratch_shapes=[pltpu.VMEM((length, width), jnp.float32), pltpu.SemaphoreType.DMA((2, length // BLOCK + 1))],
        compiler_params=PARAMS,
        name="ends",
    )(*placed(pltpu.HBM, fade_rate[0], update_in[0], norm_gain[None]))

    def local(mine, blocks, *others):
        half = pltpu.VMEM((BLOCK, width), jnp.bfloat16)
        return call(
            functools.partial(local_kernel, mine, blocks),
            [pltpu.VMEM((6 * BLOCK + 8, width), jnp.float32)],
            earlier,
            spent,
            push,
            stats,
            *others,
            scratch=[half, half],
            aliases={4: 0} if others else {},
        )[0]

    fields_0 = local(0, (0, 1))
    fields = local(1, (1,), local(1, (0,)))
    other_0 = moved(own, lambda z, y_lo, core, y_hi, x: (z, y_lo if core else 1 - y_lo, 1 - core, y_hi, x))
    other_1 = moved(own, lambda z, y_lo, core, y_hi, x: (z, 1 - y_lo, core, y_hi, x))
    partner = between_cores(own)
    neighbour, *sends = call(pair_kernel, [packet, tile, tile, tile], own, partner, other_1, other_0)
    around = [relayed(send, lambda z, y_lo, y_hi, x, to=to: (to[z], y_lo, y_hi, x)) for send, to in zip(sends, Z_ROUND)]
    (entering,) = call(entering_kernel, [packet], *around, neighbour)
    sent = between_cores(fields_0)
    came = between_cores(entering)
    states, power = call(power_kernel, [full, tile], entering, own, partner, fields, stats, sent)
    (states,) = call(states_kernel, [full], came, partner, fields_0, stats, gain, states, aliases={5: 0})

    power = power + relayed(power, lambda z, y_lo, y_hi, x: (z, y_lo, 1 - y_hi, x))
    for part in [relayed(power, lambda z, y_lo, y_hi, x, to=to: (z, y_lo, y_hi, to[x])) for to in X_ROUND]:
        power = power + part
    came = between_cores(power)

    def norm(mine, power, *before):
        return pl.pallas_call(
            functools.partial(norm_kernel, mine, float(total_length) ** -0.5, width * chan),
            out_shape=jax.ShapeDtypeStruct((length, width), jnp.bfloat16),
            in_specs=[VMEM] * 3 + [HBM] * len(before),
            out_specs=HBM,
            input_output_aliases={3: 0} if before else {},
            scratch_shapes=[pltpu.VMEM((length, width), jnp.bfloat16), pltpu.SemaphoreType.DMA((4,))],
            compiler_params=PARAMS,
        )(*placed(pltpu.VMEM, power, states, gain), *placed(pltpu.HBM, *before))

    return norm(0, came, norm(1, power))[None]


def solution(mesh):
    shard = P(None, "time", "chan")
    return jax.shard_map(per_device, mesh=mesh, in_specs=(shard, shard, P("chan")), out_specs=shard, check_vma=False)
```

```python
import functools
import math

import jax
import jax.numpy as jnp
from jax import lax
from jax.experimental import pallas as pl
from jax.experimental.pallas import tpu as pltpu
from jax.sharding import PartitionSpec as P


LANES = 128
BLOCK = 256
Z_ROUND = ((1, 3, 0, 2), (3, 2, 1, 0), (2, 0, 3, 1))
X_ROUND = ((1, 3, 0, 2), (3, 2, 1, 0), (2, 0, 3, 1))


def dot(a, b):
    return jnp.dot(a, b, preferred_element_type=jnp.float32)


def rows_of(row):
    return [row[:, k : k + LANES] for k in range(0, row.shape[1], LANES)]


def triangle(keeps):
    shape = (BLOCK, BLOCK)
    kept = keeps(lax.broadcasted_iota(jnp.int32, shape, 0), lax.broadcasted_iota(jnp.int32, shape, 1))
    return jnp.where(kept, 1.0, 0.0).astype(jnp.bfloat16)


def wide(tile):
    return jnp.concatenate([tile[k : k + 1] for k in range(4)], axis=1)


def my_place():
    me = lax.axis_index("time")
    return me // 4, (me // 2) % 2, me % 2


def unpacked(packet):
    first, second = packet[:8], packet[8:]
    return first, pltpu.roll(first, 4, axis=0), second


def packed(keep, forward, backward):
    return jnp.concatenate([keep[:4], forward[:4], backward[:4], keep[:4]], axis=0)


def joined(earlier, later):
    keep_0, forward_0, backward_0 = earlier
    keep_1, forward_1, backward_1 = later
    return keep_0 * keep_1, keep_1 * forward_0 + forward_1, backward_0 + keep_0 * backward_1


def chosen(take, yes, no):
    return tuple(jnp.where(take, a, b) for a, b in zip(yes, no))


def ends_kernel(per_rate, rate_hbm, update_hbm, gain_hbm, earlier, spent, push, stats, packet, gain, rate, arrived):
    blocks = rate.shape[0] // BLOCK
    copies = []
    for k in range(blocks):
        span = pl.ds(k * BLOCK, BLOCK)
        copies.append(pltpu.make_async_copy(rate_hbm.at[span], rate.at[span], arrived.at[0, k]))
        copies.append(pltpu.make_async_copy(update_hbm.at[span], push.at[span], arrived.at[1, k]))
    copies.append(pltpu.make_async_copy(gain_hbm, gain, arrived.at[0, blocks]))
    for copy in copies:
        copy.start()
    half = BLOCK // 2
    line = lax.broadcasted_iota(jnp.int32, (half, BLOCK), 0)
    column = lax.broadcasted_iota(jnp.int32, (half, BLOCK), 1) % half
    twice_lower = jnp.where(line >= column, 1.0, 0.0).astype(jnp.bfloat16)
    ends = []
    for k in range(blocks):
        copies[2 * k].wait()
        so_far = 0.0
        for row in range(k * BLOCK, (k + 1) * BLOCK, half):
            span = pl.ds(row, half)
            step = rate[span, :] * per_rate
            high = step.astype(jnp.bfloat16)
            low = (step - high.astype(jnp.float32)).astype(jnp.bfloat16)
            total = dot(twice_lower, jnp.concatenate([high, low], axis=0)) + so_far
            spent[span, :] = total
            earlier[span, :] = total - rate[span, :] * per_rate
            so_far = spent[pl.ds(row + half - 8, 8), :][7:]
        copies[2 * k + 1].wait()
        forward = jnp.zeros((8, rate.shape[1]), jnp.float32)
        backward = forward
        for row in range(k * BLOCK, (k + 1) * BLOCK, 16):
            rows = pl.ds(row, 16)
            total = spent[rows, :]
            update = push[rows, :].astype(jnp.float32)
            more = jnp.exp2(total) * update
            less = jnp.exp2(-earlier[rows, :]) * update
            forward = forward + (more[:8] + more[8:])
            backward = backward + (less[:8] + less[8:])
        keep = jnp.exp2(-spent[pl.ds((k + 1) * BLOCK - 8, 8), :][7:])
        ends.append((keep, keep * jnp.sum(forward, axis=0, keepdims=True), jnp.sum(backward, axis=0, keepdims=True)))
    keep, forward, backward = joined(*ends)
    copies[-1].wait()
    row = ends[0][0]
    stats[...] = jnp.concatenate([ends[0][0], ends[0][1], ends[1][0], ends[1][2], row, row, row, row], axis=0)
    packet[...] = jnp.concatenate(rows_of(keep) + rows_of(forward) + rows_of(backward) + rows_of(keep), axis=0)


def field(fields, block, k):
    return fields.at[pl.ds((3 * block + k) * BLOCK, BLOCK)]


def local_kernel(mine, blocks, earlier, spent, push, stats, *refs):
    fields, ahead, behind = refs[-3:]

    @pl.when(my_place()[2] == mine)
    def _():
        lower, upper = triangle(jnp.greater_equal), triangle(jnp.less_equal)
        for block in blocks:
            local, fall, rise = (field(fields, block, k) for k in range(3))
            for row in range(0, BLOCK, 16):
                rows, here = pl.ds(block * BLOCK + row, 16), pl.ds(row, 16)
                total = spent[rows, :]
                before = earlier[rows, :]
                update = push[rows, :].astype(jnp.float32)
                fall[here, :] = jnp.exp2(-total)
                rise[here, :] = jnp.exp2(before)
                ahead[here, :] = ((jnp.exp2(total) - 1.0) * update).astype(jnp.bfloat16)
                behind[here, :] = ((jnp.exp2(-before) - 1.0) * update).astype(jnp.bfloat16)
            update = push[pl.ds(block * BLOCK, BLOCK), :]
            sums = dot(lower, update) + dot(lower, ahead[...])
            later = dot(upper, update) + dot(upper, behind[...])
            local[...] = fall[...] * sums + rise[...] * later
        if len(blocks) == 2:
            fields[pl.ds(6 * BLOCK, 8), :] = stats[...]


def table(values, place):
    chosen_value = jnp.int32(values[-1])
    for k, value in enumerate(values[:-1]):
        chosen_value = jnp.where(place == k, value, chosen_value)
    return chosen_value


def pair_kernel(own, partner, other_1, other_0, neighbour, *sends):
    z, y_lo, _ = my_place()
    chip = joined(unpacked(partner[...]), unpacked(own[...]))
    other = joined(unpacked(other_0[...]), unpacked(other_1[...]))
    neighbour[...] = packed(*other)
    second = y_lo == 1
    keep, forward, backward = joined(chosen(second, other, chip), chosen(second, chip, other))
    for places, send in zip(Z_ROUND, sends):
        send[...] = jnp.concatenate([keep[:4], jnp.where(table(places, z) > z, forward, backward)[:4]], axis=0)


def entering_kernel(came_0, came_1, came_2, neighbour, entering):
    z, y_lo, _ = my_place()
    packets = [ref[...] for ref in (came_0, came_1, came_2)]
    sources = [table([places.index(k) for k in range(4)], z) for places in Z_ROUND]
    before = jnp.zeros((8, LANES), jnp.float32)
    after = before
    ordered = []
    for k in range(4):
        packet = packets[0]
        for source, other in zip(sources[1:], packets[1:]):
            packet = jnp.where(source == k, other, packet)
        ordered.append((packet, pltpu.roll(packet, 4, axis=0)))
    for k in range(4):
        keep, forward = ordered[k]
        before = jnp.where(k < z, keep * before + forward, before)
        keep, backward = ordered[3 - k]
        after = jnp.where(3 - k > z, keep * after + backward, after)
    keep, forward, backward = unpacked(neighbour[...])
    before = jnp.where(y_lo == 1, keep * before + forward, before)
    after = jnp.where(y_lo == 0, keep * after + backward, after)
    entering[...] = jnp.concatenate([before, after], axis=0)


def entering_blocks(before, after, stats):
    before, after = wide(before), wide(after)
    keep_0, forward_0, keep_1, backward_1 = (stats[k : k + 1, :] for k in range(4))
    return (before, keep_0 * (keep_1 * after + backward_1)), (keep_0 * before + forward_0, keep_1 * after)


def filtered(fields, entering, use):
    for k in range(2 * BLOCK // 8):
        block, row = divmod(8 * k, BLOCK)
        local, fall, rise = (field(fields, block, j)[pl.ds(row, 8), :] for j in range(3))
        first, second = entering[block]
        use(k, local + fall * first + rise * second)


def power_kernel(entering, own, partner, fields, stats, fields_0, states, power_out):
    core = my_place()[2]

    @pl.when(core == 0)
    def _():
        power_out[...] = jnp.zeros((8, LANES), jnp.float32)

    @pl.when(core == 1)
    def _():
        before, after = entering[:8], entering[8:]
        lane = lax.broadcasted_iota(jnp.int32, (8, LANES), 1)
        power = [jnp.zeros((8, LANES), jnp.float32)]

        def add(place, state):
            square = functools.reduce(jnp.add, rows_of(state * state))
            power[0] = jnp.where(lane == place, jnp.sum(square, axis=1, keepdims=True), power[0])

        def keep_it(k, state):
            states[pl.ds(8 * k, 8), :] = state
            add(LANES // 2 + k, state)

        keep, forward, _ = unpacked(partner[...])
        filtered(fields, entering_blocks(keep * before + forward, after, stats), keep_it)
        keep, _, backward = unpacked(own[...])
        stats_0 = fields_0[pl.ds(6 * BLOCK, 8), :]
        filtered(fields_0, entering_blocks(before, keep * after + backward, stats_0), add)
        power_out[...] = power[0]


def states_kernel(came, partner, fields, stats, gain, states_1, states):
    @pl.when(my_place()[2] == 0)
    def _():
        before, after = came[:8], came[8:]
        keep, _, backward = unpacked(partner[...])
        scale = gain[...]

        def keep_it(k, state):
            states[pl.ds(8 * k, 8), :] = state * scale

        filtered(fields, entering_blocks(before, keep * after + backward, stats), keep_it)


def norm_kernel(mine, scale, channels, power, states, gain, *refs):
    mixed_hbm, mixed, left = refs[-3:]

    @pl.when(my_place()[2] == mine)
    def _():
        factor = lax.rsqrt(power[...] * (scale * scale / channels) + 1e-6) * scale
        gains = gain[...]
        pieces = left.shape[0]
        height = states.shape[0] // pieces
        copies = []
        for piece in range(pieces):
            for k in range(piece * height // 16, (piece + 1) * height // 16):
                halves = []
                for j in (2 * k, 2 * k + 1):
                    place = j + mine * (LANES // 2)
                    half = states[pl.ds(8 * j, 8), :] * factor[:, place : place + 1]
                    halves.append(half * gains if mine else half)
                mixed[pl.ds(16 * k, 16), :] = jnp.concatenate(halves, axis=0).astype(jnp.bfloat16)
            span = pl.ds(piece * height, height)
            copy = pltpu.make_async_copy(mixed.at[span], mixed_hbm.at[span], left.at[piece])
            copy.start()
            copies.append(copy)
        for copy in copies:
            copy.wait()


VMEM = pl.BlockSpec(memory_space=pltpu.VMEM)
HBM = pl.BlockSpec(memory_space=pltpu.HBM)
PARAMS = pltpu.CompilerParams(vmem_limit_bytes=16 << 20)
SPACES = ("time", "chan")


def placed(space, *arrays):
    return [pltpu.with_memory_space_constraint(array, space) for array in arrays]


def call(kernel, outs, *arrays, scratch=(), aliases={}):
    return pl.pallas_call(
        kernel,
        out_shape=tuple(outs),
        in_specs=[VMEM] * len(arrays),
        out_specs=(VMEM,) * len(outs),
        scratch_shapes=scratch,
        input_output_aliases=aliases,
        compiler_params=PARAMS,
    )(*placed(pltpu.VMEM, *arrays))


def moved(value, target):
    pairs = []
    for place in range(128):
        t, c = place // 8, place % 8
        z, y_lo, core, y_hi, x = target(t // 4, (t // 2) % 2, t % 2, c // 4, c % 4)
        pairs.append((place, (z * 4 + y_lo * 2 + core) * 8 + y_hi * 4 + x))
    return lax.ppermute(value, SPACES, pairs)


def between_cores(value):
    return moved(
        value, lambda z, y_lo, core, y_hi, x: (z, y_lo, 1 - core, y_hi, x))


def relayed(value, target):
    return moved(
        value,
        lambda z, y_lo, core, y_hi, x: (
            (*target(z, y_lo, y_hi, x)[:2], 1, *target(z, y_lo, y_hi, x)[2:]) if core else (z, 1 - y_lo, 0, y_hi, x)
        ),
    )


def per_device(fade_rate, update_in, norm_gain):
    time, chan = lax.axis_size("time"), lax.axis_size("chan")
    length, width = fade_rate.shape[1:]
    total_length = length * time
    per_rate = math.log2(math.e) / total_length
    full = pltpu.VMEM((length, width), jnp.float32)
    packet = pltpu.VMEM((16, LANES), jnp.float32)
    tile = pltpu.VMEM((8, LANES), jnp.float32)
    earlier, spent, push, stats, own, gain = pl.pallas_call(
        functools.partial(ends_kernel, per_rate),
        out_shape=(
            full,
            full,
            pltpu.VMEM((length, width), jnp.bfloat16),
            pltpu.VMEM((8, width), jnp.float32),
            packet,
            pltpu.VMEM((1, width), jnp.float32),
        ),
        in_specs=[HBM] * 3,
        out_specs=(VMEM,) * 6,
        scratch_shapes=[pltpu.VMEM((length, width), jnp.float32), pltpu.SemaphoreType.DMA((2, length // BLOCK + 1))],
        compiler_params=PARAMS,
        name="ends",
    )(*placed(pltpu.HBM, fade_rate[0], update_in[0], norm_gain[None]))

    def local(mine, blocks, *others):
        half = pltpu.VMEM((BLOCK, width), jnp.bfloat16)
        return call(
            functools.partial(local_kernel, mine, blocks),
            [pltpu.VMEM((6 * BLOCK + 8, width), jnp.float32)],
            earlier,
            spent,
            push,
            stats,
            *others,
            scratch=[half, half],
            aliases={4: 0} if others else {},
        )[0]

    fields_0 = local(0, (0, 1))
    fields = local(1, (1,), local(1, (0,)))
    other_0 = moved(own, lambda z, y_lo, core, y_hi, x: (z, y_lo if core else 1 - y_lo, 1 - core, y_hi, x))
    other_1 = moved(own, lambda z, y_lo, core, y_hi, x: (z, 1 - y_lo, core, y_hi, x))
    partner = between_cores(own)
    neighbour, *sends = call(pair_kernel, [packet, tile, tile, tile], own, partner, other_1, other_0)
    around = [relayed(send, lambda z, y_lo, y_hi, x, to=to: (to[z], y_lo, y_hi, x)) for send, to in zip(sends, Z_ROUND)]
    (entering,) = call(entering_kernel, [packet], *around, neighbour)
    sent = between_cores(fields_0)
    came = between_cores(entering)
    states, power = call(power_kernel, [full, tile], entering, own, partner, fields, stats, sent)
    (states,) = call(states_kernel, [full], came, partner, fields_0, stats, gain, states, aliases={5: 0})

    power = power + relayed(power, lambda z, y_lo, y_hi, x: (z, y_lo, 1 - y_hi, x))
    for part in [relayed(power, lambda z, y_lo, y_hi, x, to=to: (z, y_lo, y_hi, to[x])) for to in X_ROUND]:
        power = power + part
    came = between_cores(power)

    def norm(mine, power, *before):
        return pl.pallas_call(
            functools.partial(norm_kernel, mine, float(total_length) ** -0.5, width * chan),
            out_shape=jax.ShapeDtypeStruct((length, width), jnp.bfloat16),
            in_specs=[VMEM] * 3 + [HBM] * len(before),
            out_specs=HBM,
            input_output_aliases={3: 0} if before else {},
            scratch_shapes=[pltpu.VMEM((length, width), jnp.bfloat16), pltpu.SemaphoreType.DMA((2,))],
            compiler_params=PARAMS,
        )(*placed(pltpu.VMEM, power, states, gain), *placed(pltpu.HBM, *before))

    return norm(0, came, norm(1, power))[None]


def solution(mesh):
    shard = P(None, "time", "chan")
    return jax.shard_map(per_device, mesh=mesh, in_specs=(shard, shard, P("chan")), out_specs=shard, check_vma=False)
```
